256 devices in a mesh: dp: 4 (over x_hi, core), mp: 64 (over x_lo, y, z).
Axes of the slice: x: 4 (x_hi: 2, x_lo: 2; x = x_hi * 2 + x_lo), y: 4, z: 8, core: 2. Of those that a mesh axis runs over, the one named last changes fastest.
Arguments:
- source_prompts: bfloat16 [128, 64, 4096], P(None, None, 'mp'), may hold values from -6 to 6
- task_logits: float32 [8, 128], replicated, may hold values from -8 to 260
- task_ids: int32 [256], P('dp'), may hold values from 0 to 7
- key_weight: bfloat16 [4096, 4096], P(None, 'mp'), may hold values from -0.09375 to 0.09375
- value_weight: bfloat16 [4096, 4096], P(None, 'mp'), may hold values from -0.09375 to 0.09375
- queries: bfloat16 [256, 128, 4096], P(('dp', 'mp')), may hold values from -32 to 32
- keys: bfloat16 [256, 128, 4096], P(('dp', 'mp')), may hold values from -16 to 16
- values: bfloat16 [256, 128, 4096], P(('dp', 'mp')), may hold values from -6 to 6
- cotangent: bfloat16 [256, 128, 4096], P(('dp', 'mp')), may hold values from -6 to 6
Outputs:
- attended: bfloat16 [256, 128, 4096], P(('dp', 'mp'))
- source_grad: float32 [128, 64, 4096], P(None, 'dp', 'mp')
- logits_grad: float32 [8, 128], replicated
The draws below stay inside these ranges and needn't reach their ends.
All inputs are finite; a program needn't handle non-finite values.
Results may differ from the reference program's by a relative error of at most 0.011.
Values may be sent and summed in bfloat16 or wider, within the bound.
No kernel may reach another device: no remote copies, remote signals or barrier semaphores. Data moves between devices by JAX's collectives and lax.ppermute only.
A program may use at most 128 MiB of HBM per device.

```python
import jax
import jax.numpy as jnp
from jax import lax

D = 4096
HEADS = 32
DH = 128
NSRC = 128
NTASK = 8
PTOK = 64
SEQ = 128
EXAMPLES = 256


def query_key_pair(key):
    paired_key = jax.random.fold_in(key, 11)
    query_seed, key_seed = jax.random.split(paired_key, 2)
    full_shape = (EXAMPLES, SEQ, D)
    query_draw = jax.random.normal(query_seed, full_shape, jnp.float32)
    key_draw = jax.random.normal(key_seed, full_shape, jnp.float32)
    return (jnp.clip(query_draw, -32.0, 32.0), jnp.clip(key_draw, -16.0, 16.0))


def draw_queries(key, part):
    return query_key_pair(key)[0].astype(jnp.bfloat16)


def draw_keys(key, part):
    return query_key_pair(key)[1].astype(jnp.bfloat16)


def draw_task_logits(key, part):
    logit_key = jax.random.fold_in(key, 23)
    base_seed = jax.random.fold_in(logit_key, 0)
    logits = jnp.clip(2.0 * jax.random.normal(base_seed, (NTASK, NSRC), jnp.float32), -8.0, 8.0)
    return logits


def plant(result, own_key, smallest, high):
    place = [jax.random.randint(jax.random.fold_in(own_key, axis), (), 0, length) for axis, length in enumerate(result.shape)]
    main_axis = result.shape.index(max(result.shape))
    beside = place[:main_axis] + [(place[main_axis] + 1) % result.shape[main_axis]] + place[main_axis + 1:]
    return result.at[tuple(place)].set(smallest).at[tuple(beside)].set(high)


def steps_of(rng, extent, cuts, least, largest):
    level, own = 1.0, jax.random.fold_in(rng, 6)
    for dim, blocks in cuts:
        steps = jnp.exp(jax.random.uniform(jax.random.fold_in(own, dim), (blocks,), jnp.float32, least / len(cuts), largest / len(cuts)))
        level = level * jnp.repeat(steps, extent[dim] // blocks).reshape([-1 if axis == dim else 1 for axis in range(len(extent))])
    return level


def centred(own_key, shape, scale, limit, pieces=(), kind=jnp.bfloat16):
    loudness = steps_of(own_key, shape, pieces, -0.22, 0.18) if pieces else 1.0
    drawn = jax.random.normal(own_key, shape, jnp.float32) * scale * loudness
    return jnp.minimum(jnp.maximum(drawn, -limit), limit).astype(kind)


def setup_inputs(seed: int = 0) -> dict:
    streams_of = jax.random.split(jax.random.key(seed), 10)
    return {
        "source_prompts": centred(streams_of[0], (NSRC, PTOK, D), 1.0, 6.0, ((2, 64),)),
        "task_logits": draw_task_logits(jax.random.fold_in(streams_of[9], 71), 0),
        "task_ids": plant(jax.random.randint(streams_of[2], (EXAMPLES,), 0, NTASK), jax.random.fold_in(streams_of[2], 1), 0, NTASK - 1).astype(jnp.int32),
        "key_weight": centred(streams_of[3], (D, D), D ** -0.5, 0.09375, ((1, 64),)),
        "value_weight": centred(streams_of[4], (D, D), D ** -0.5, 0.09375, ((1, 64),)),
        "queries": draw_queries(jax.random.fold_in(streams_of[9], 71), 0),
        "keys": draw_keys(jax.random.fold_in(streams_of[9], 71), 0),
        "values": centred(streams_of[7], (EXAMPLES, SEQ, D), 1.0, 6.0, ((0, 256),)),
        "cotangent": centred(streams_of[8], (EXAMPLES, SEQ, D), 1.0, 6.0, ((0, 256),)),
    }


mask_fill = -1.0e30


def example_pass(prompt_pair, query_rows, key_rows, value_rows, cot_rows):
    score_scale = DH ** -0.5
    key_all = jnp.concatenate([prompt_pair[:, 0, :], key_rows], axis=0)
    value_all = jnp.concatenate([prompt_pair[:, 1, :], value_rows], axis=0)
    query_heads = query_rows.astype(jnp.float32).reshape(SEQ, HEADS, DH)
    key_heads = key_all.astype(jnp.float32).reshape(PTOK + SEQ, HEADS, DH)
    value_heads = value_all.astype(jnp.float32).reshape(PTOK + SEQ, HEADS, DH)
    cot_heads = cot_rows.astype(jnp.float32).reshape(SEQ, HEADS, DH)
    scores = jnp.einsum("ihd,jhd->hij", query_heads, key_heads) * score_scale
    column = jnp.arange(PTOK + SEQ)[None, :]
    position = jnp.arange(SEQ)[:, None]
    visible = (column < PTOK) | (column - PTOK <= position)
    scores = jnp.where(visible[None], scores, mask_fill)
    top_score = jnp.max(scores, axis=2, keepdims=True)
    exponent = jnp.exp(scores - top_score)
    attention = exponent / jnp.sum(exponent, axis=2, keepdims=True)
    attention_rounded = attention.astype(jnp.bfloat16)
    attended = jnp.einsum("hij,jhd->ihd", attention_rounded.astype(jnp.float32), value_heads)
    attended = attended.astype(jnp.bfloat16).reshape(SEQ, D)
    grad_attention = jnp.einsum("ihd,jhd->hij", cot_heads, value_heads)
    inner_sum = jnp.sum(attention * grad_attention, axis=2, keepdims=True)
    grad_scores = (attention * (grad_attention - inner_sum)).astype(jnp.bfloat16)
    key_grads = jnp.einsum("hij,ihd->jhd", grad_scores[:, :, :PTOK].astype(jnp.float32), query_heads)
    key_grads = (key_grads * score_scale).astype(jnp.bfloat16)
    value_grads = jnp.einsum("hij,ihd->jhd", attention_rounded[:, :, :PTOK].astype(jnp.float32), cot_heads)
    value_grads = value_grads.astype(jnp.bfloat16)
    return attended, jnp.stack([key_grads.reshape(PTOK, D), value_grads.reshape(PTOK, D)], axis=1)


def reference(source_prompts, task_logits, task_ids, key_weight, value_weight, queries, keys, values, cotangent):
    mix_weights = jax.nn.softmax(task_logits, axis=1)
    mix_rounded = mix_weights.astype(jnp.bfloat16)
    mixture = jnp.dot(mix_rounded, source_prompts.reshape(NSRC, PTOK * D), preferred_element_type=jnp.float32)
    mixture = mixture.astype(jnp.bfloat16).reshape(NTASK * PTOK, D)
    prompt_keys = jnp.dot(mixture, key_weight, preferred_element_type=jnp.float32).astype(jnp.bfloat16)
    prompt_values = jnp.dot(mixture, value_weight, preferred_element_type=jnp.float32).astype(jnp.bfloat16)
    prompt_table = jnp.stack([prompt_keys, prompt_values], axis=1).reshape(NTASK, PTOK, 2, D)

    def one_example(packed):
        task_index, query_rows, key_rows, value_rows, cot_rows = packed
        prompt_pair = lax.dynamic_index_in_dim(prompt_table, task_index, 0, keepdims=False)
        return example_pass(prompt_pair, query_rows, key_rows, value_rows, cot_rows)

    attended, prompt_grads = lax.map(one_example, (task_ids, queries, keys, values, cotangent))
    selector = (task_ids[:, None] == jnp.arange(NTASK, dtype=jnp.int32)[None, :]).astype(jnp.float32)
    task_grads = jnp.dot(selector.T, prompt_grads.reshape(EXAMPLES, PTOK * 2 * D).astype(jnp.float32),
                         precision=lax.Precision.HIGHEST)
    task_grads = task_grads.reshape(NTASK * PTOK, 2, D)
    mixture_grad = jnp.dot(task_grads[:, 0, :], key_weight.astype(jnp.float32).T, precision=lax.Precision.HIGHEST)
    mixture_grad = mixture_grad + jnp.dot(task_grads[:, 1, :], value_weight.astype(jnp.float32).T,
                                          precision=lax.Precision.HIGHEST)
    mixture_grad = mixture_grad.reshape(NTASK, PTOK * D)
    source_grad = jnp.dot(mix_weights.T, mixture_grad, precision=lax.Precision.HIGHEST).reshape(NSRC, PTOK, D)
    weight_grad = jnp.dot(mixture_grad, source_prompts.reshape(NSRC, PTOK * D).astype(jnp.float32).T,
                          precision=lax.Precision.HIGHEST)
    logits_grad = mix_weights * (weight_grad - jnp.sum(mix_weights * weight_grad, axis=1, keepdims=True))
    return attended, source_grad, logits_grad
```

```python
import functools

import jax
import jax.numpy as jnp
from jax import lax
from jax.experimental import pallas as pl
from jax.experimental.pallas import tpu as pltpu
from jax.sharding import Mesh
from jax.sharding import PartitionSpec as P

D = 4096
HEADS = 32
DH = 128
NSRC = 128
NTASK = 8
PTOK = 64
SEQ = 128
DP = ("dp_0", "dp_1")
MP = ("mp_0", "mp_1", "mp_2")
DP_MP = ("dp_0", "dp_1", "mp_0", "mp_1", "mp_2")
XY = ("mp_0", "mp_1")
XYC = ("dp_0", "dp_1", "mp_0", "mp_1")
GROUPS = 4
ROWS = PTOK // GROUPS
NXY = 8
NZ = 8
COLS = D // (NXY * NZ)
TROWS = NTASK * ROWS
BF = jnp.bfloat16
F32 = jnp.float32


SMEM = pl.BlockSpec(memory_space=pltpu.SMEM)
VMEM = pl.BlockSpec(memory_space=pltpu.VMEM)


def dot(a, b, ca, cb):
    return lax.dot_general(a, b, (((ca,), (cb,)), ((), ())), preferred_element_type=F32)


def iota(shape, axis):
    return lax.broadcasted_iota(jnp.int32, shape, axis)


def lane_swap(a):
    return pltpu.roll(a, COLS, a.ndim - 1)


def mixture_kernel(meta, logits_ref, prompts_ref, mix_ref, out_ref):
    logits = logits_ref[...]
    exponent = jnp.exp(logits - jnp.max(logits, axis=1, keepdims=True))
    mix = exponent / jnp.sum(exponent, axis=1, keepdims=True)
    mix_ref[...] = mix
    spread_rows = (iota((TROWS, NTASK), 0) // ROWS == iota((TROWS, NTASK), 1)).astype(BF)
    by_row = dot(spread_rows, mix.astype(BF), 1, 0).astype(BF)
    wide = NSRC * ROWS
    spread_cols = (iota((NSRC, wide), 1) // ROWS == iota((NSRC, wide), 0)).astype(BF)
    spread = dot(by_row, spread_cols, 1, 0)
    same = iota((TROWS, wide), 0) % ROWS == iota((TROWS, wide), 1) % ROWS
    left = jnp.where(same, spread, 0.0).astype(BF)
    rows = prompts_ref[...].reshape(wide, COLS)
    mixture = dot(left, rows, 1, 0)
    padded = jnp.concatenate([mixture, jnp.zeros_like(mixture)], axis=1)
    turned = padded.T[:COLS].astype(BF)
    for k in range(NZ):
        out_ref[k] = turned


def make_mixture(meta, logits, prompts):
    return pl.pallas_call(
        mixture_kernel,
        grid_spec=pltpu.PrefetchScalarGridSpec(
            num_scalar_prefetch=1,
            grid=(1,),
            in_specs=[
                pl.BlockSpec((NTASK, NSRC), lambda i, m: (0, 0)),
                pl.BlockSpec((NSRC, ROWS, COLS), lambda i, m: (0, m[0], 0)),
            ],
            out_specs=[
                pl.BlockSpec((NTASK, NSRC), lambda i, m: (0, 0)),
                pl.BlockSpec((NZ, COLS, TROWS), lambda i, m: (0, 0, 0)),
            ],
        ),
        out_shape=[
            jax.ShapeDtypeStruct((NTASK, NSRC), F32),
            jax.ShapeDtypeStruct((NZ, COLS, TROWS), BF),
        ],
    )(meta, logits, prompts)


def project_kernel(meta, *refs):
    blocks, (key_ref, value_ref, out_ref) = refs[:NXY], refs[NXY:]
    span = NZ * COLS
    keys = jnp.zeros((TROWS, COLS), F32)
    values = jnp.zeros((TROWS, COLS), F32)
    for k in range(NXY):
        start = pl.multiple_of((meta[1] ^ k) * span, span)
        rows = blocks[k][...].T
        keys += dot(rows, key_ref[pl.ds(start, span), :], 1, 0)
        values += dot(rows, value_ref[pl.ds(start, span), :], 1, 0)
    both = jnp.concatenate([keys, values], axis=1).astype(BF)
    for k in range(NZ):
        out_ref[k] = both


def project(meta, blocks, key_weight, value_weight):
    return pl.pallas_call(
        project_kernel,
        in_specs=[SMEM] + [VMEM] * (NXY + 2),
        out_specs=VMEM,
        out_shape=jax.ShapeDtypeStruct((NZ, TROWS, 2 * COLS), BF),
    )(meta, *blocks, key_weight, value_weight)


def select_kernel(meta, i0, i1, i2, i3, in_ref, out_ref, table_ref):
    low = iota((NTASK, ROWS, 2 * COLS), 2) < COLS
    for h in range(NZ // 2):
        even = in_ref[2 * h].astype(F32)
        odd = in_ref[2 * h + 1].astype(F32)
        table_ref[:, h] = jnp.where(low, even, lane_swap(odd)).astype(BF)
        table_ref[:, NZ // 2 + h] = jnp.where(low, lane_swap(even), odd).astype(BF)
    group, z = meta[0], meta[2]
    for k, ids in enumerate((i0, i1, i2, i3)):
        for j in range(NXY):
            out_ref[(group ^ k) * NXY + j] = table_ref[ids[j * NZ + z]]


def select_prompts(meta, ids, gathered):
    return pl.pallas_call(
        select_kernel,
        in_specs=[SMEM] * 5 + [VMEM],
        out_specs=VMEM,
        out_shape=jax.ShapeDtypeStruct((GROUPS * NXY, NZ, ROWS, 2 * COLS), BF),
        scratch_shapes=[pltpu.VMEM((NTASK, NZ, ROWS, 2 * COLS), BF)],
    )(meta, *ids, gathered)


def attention_kernel(prompt_ref, q_ref, k_ref, v_ref, c_ref, att_ref, grad_ref):
    scale = DH ** (-0.5)
    visible = iota((SEQ, SEQ), 0) <= iota((SEQ, SEQ), 1)
    for h in range(NZ // 2):
        at = slice(h * DH, (h + 1) * DH)
        q, k, v, c = q_ref[:, at], k_ref[:, at], v_ref[:, at], c_ref[:, at]
        kp = prompt_ref[:, 0, h].reshape(PTOK, DH)
        vp = prompt_ref[:, 0, NZ // 2 + h].reshape(PTOK, DH)
        sp = dot(kp, q, 1, 1) * scale
        so = jnp.where(visible, dot(k, q, 1, 1) * scale, -1e30)
        top = jnp.maximum(jnp.max(sp, axis=0, keepdims=True), jnp.max(so, axis=0, keepdims=True))
        ep, eo = jnp.exp(sp - top), jnp.exp(so - top)
        total = jnp.sum(ep, axis=0, keepdims=True) + jnp.sum(eo, axis=0, keepdims=True)
        share = 1.0 / total
        ap, ao = ep * share, eo * share
        apb, aob = ap.astype(BF), ao.astype(BF)
        att = dot(apb, vp, 0, 0) + dot(aob, v, 0, 0)
        att_ref[:, at] = att.astype(BF)
        gp, go = dot(vp, c, 1, 1), dot(v, c, 1, 1)
        inner = jnp.sum(ap * gp, axis=0, keepdims=True) + jnp.sum(ao * go, axis=0, keepdims=True)
        gs = (ap * (gp - inner)).astype(BF)
        kg = (dot(gs, q, 1, 0) * scale).astype(BF)
        vg = dot(apb, c, 1, 0).astype(BF)
        grad_ref[:, 0, h] = kg.reshape(GROUPS, ROWS, DH)
        grad_ref[:, 0, NZ // 2 + h] = vg.reshape(GROUPS, ROWS, DH)


def attention(prompts, queries, keys, values, cotangent):
    wide = DH * NZ // 2
    seq = pl.BlockSpec((None, SEQ, wide), lambda i: (0, 0, i))
    pair = pl.BlockSpec((GROUPS, 1, NZ, ROWS, DH), lambda i: (0, i, 0, 0, 0))
    return pl.pallas_call(
        attention_kernel,
        grid=(NXY,),
        in_specs=[pair, seq, seq, seq, seq],
        out_specs=[seq, pair],
        out_shape=[
            jax.ShapeDtypeStruct((1, SEQ, D), BF),
            jax.ShapeDtypeStruct((GROUPS, NXY, NZ, ROWS, DH), BF),
        ],
    )(prompts, queries, keys, values, cotangent)


def tasks_kernel(meta, i0, i1, i2, i3, in_ref, out_ref, total_ref):
    total_ref[...] = jnp.zeros_like(total_ref)
    group, z = meta[0], meta[2]
    for k, ids in enumerate((i0, i1, i2, i3)):
        for j in range(NXY):
            total_ref[ids[j * NZ + z]] += in_ref[(group ^ k) * NXY + j].astype(F32)
    low = iota((NTASK, ROWS, 2 * COLS), 2) < COLS
    for h in range(NZ // 2):
        kg, vg = total_ref[:, h], total_ref[:, NZ // 2 + h]
        out_ref[2 * h] = jnp.where(low, kg, lane_swap(vg)).astype(BF)
        out_ref[2 * h + 1] = jnp.where(low, lane_swap(kg), vg).astype(BF)


def sum_by_task(meta, ids, incoming):
    return pl.pallas_call(
        tasks_kernel,
        in_specs=[SMEM] * 5 + [VMEM],
        out_specs=VMEM,
        out_shape=jax.ShapeDtypeStruct((NZ, NTASK, ROWS, 2 * COLS), BF),
        scratch_shapes=[pltpu.VMEM((NTASK, NZ, ROWS, 2 * COLS), F32)],
    )(meta, *ids, incoming)


def rows_kernel(in_ref, key_ref, value_ref, out_ref):
    grads = in_ref[0].astype(F32)
    for k in range(1, NZ):
        grads += in_ref[k].astype(F32)
    kg = grads[:, :COLS].astype(BF)
    vg = lane_swap(grads)[:, :COLS].astype(BF)
    out_ref[0] = (dot(key_ref[...], kg, 1, 1) + dot(value_ref[...], vg, 1, 1)).astype(BF)


def row_terms(parts, key_weight, value_weight):
    span = NZ * COLS
    weight = pl.BlockSpec((span, COLS), lambda i: (i, 0))
    return pl.pallas_call(
        rows_kernel,
        grid=(NXY,),
        in_specs=[pl.BlockSpec((NZ, TROWS, 2 * COLS), lambda i: (0, 0, 0)), weight, weight],
        out_specs=pl.BlockSpec((1, span, TROWS), lambda i: (i, 0, 0)),
        out_shape=jax.ShapeDtypeStruct((NXY, span, TROWS), BF),
    )(parts, key_weight, value_weight)


def last_kernel(meta, mix_sm, in_ref, prompts_ref, source_ref, weight_ref):
    tile = in_ref[0].astype(F32)
    for k in range(1, NZ):
        tile += in_ref[k].astype(F32)
    padded = jnp.concatenate([tile, jnp.zeros_like(tile)], axis=0)
    tile = padded.T[:, :COLS]
    tasks = [tile[t * ROWS : (t + 1) * ROWS] for t in range(NTASK)]
    for s in range(NSRC):
        terms = [mix_sm[t, s] * tasks[t] for t in range(NTASK)]
        while len(terms) > 1:
            terms = [a + b for a, b in zip(terms[::2], terms[1::2])]
        source_ref[s] = terms[0]
    wide = NSRC * ROWS
    rows = prompts_ref[...].reshape(wide, COLS)
    high = tile.astype(BF)
    rest = (tile - high.astype(F32)).astype(BF)
    full = dot(high, rows, 1, 1) + dot(rest, rows, 1, 1)
    same = iota((TROWS, wide), 0) % ROWS == iota((TROWS, wide), 1) % ROWS
    kept = jnp.where(same, full, 0.0).reshape(NTASK, ROWS, wide).sum(axis=1)
    gather = (iota((wide, NSRC), 0) // ROWS == iota((wide, NSRC), 1)).astype(F32)
    weight_ref[...] = jnp.dot(
        kept, gather, precision=lax.Precision.HIGHEST, preferred_element_type=F32
    )


def last_products(meta, mix, parts, prompts):
    return pl.pallas_call(
        last_kernel,
        grid_spec=pltpu.PrefetchScalarGridSpec(
            num_scalar_prefetch=1,
            grid=(1,),
            in_specs=[
                pl.BlockSpec(memory_space=pltpu.SMEM),
                pl.BlockSpec((NZ, COLS, TROWS), lambda i, m: (0, 0, 0)),
                pl.BlockSpec((NSRC, ROWS, COLS), lambda i, m: (0, m[0], 0)),
            ],
            out_specs=[
                pl.BlockSpec((NSRC, ROWS, COLS), lambda i, m: (0, 0, 0)),
                pl.BlockSpec((NTASK, NSRC), lambda i, m: (0, 0)),
            ],
        ),
        out_shape=[
            jax.ShapeDtypeStruct((NSRC, ROWS, COLS), F32),
            jax.ShapeDtypeStruct((NTASK, NSRC), F32),
        ],
    )(meta, mix, parts, prompts)


def exchange(blocks, axes):
    return lax.all_to_all(blocks, axes, split_axis=0, concat_axis=0, tiled=True)


def from_peers(array, axes, members):
    got = [array]
    for k in range(1, members):
        got.append(lax.ppermute(array, axes, [(i, i ^ k) for i in range(members)]))
    return got


def tree_sum(terms):
    while len(terms) > 1:
        terms = [a + b for a, b in zip(terms[::2], terms[1::2])]
    return terms[0]


def on_device(
    source_prompts,
    task_logits,
    task_ids,
    key_weight,
    value_weight,
    queries,
    keys,
    values,
    cotangent,
):
    meta = jnp.stack([lax.axis_index(DP), lax.axis_index(XY), lax.axis_index("mp_2")])
    meta = meta.astype(jnp.int32)
    ids = from_peers(task_ids, DP, GROUPS)
    mix, copies = make_mixture(meta, task_logits, source_prompts)
    span = exchange(copies, "mp_2").reshape(NZ * COLS, TROWS)
    blocks = from_peers(span, XY, NXY)
    copies = project(meta, blocks, key_weight, value_weight)
    gathered = exchange(copies, "mp_2").reshape(NZ, NTASK, ROWS, 2 * COLS)
    outgoing = select_prompts(meta, ids, gathered)
    prompts = exchange(outgoing, XYC).reshape(GROUPS, NXY, NZ, ROWS, DH)
    attended, grads = attention(prompts, queries, keys, values, cotangent)
    incoming = exchange(grads.reshape(GROUPS * NXY, NZ, ROWS, DH), XYC)
    by_task = sum_by_task(meta, ids, incoming).reshape(NZ, TROWS, 2 * COLS)
    parts = exchange(by_task, "mp_2")
    terms = row_terms(parts, key_weight, value_weight)
    terms = exchange(terms, XY)
    terms = terms.astype(F32).sum(axis=0).astype(BF).reshape(NZ, COLS, TROWS)
    terms = exchange(terms, "mp_2")
    source_grad, weight_part = last_products(meta, mix, terms, source_prompts)
    weight_part = tree_sum(from_peers(weight_part, XY, NXY))
    weight_part = tree_sum(from_peers(weight_part, DP, GROUPS))
    spread = jnp.broadcast_to(weight_part[None], (NZ, NTASK, NSRC))
    weight_grad = exchange(spread, "mp_2").sum(axis=0)
    logits_grad = mix * (weight_grad - jnp.sum(mix * weight_grad, axis=1, keepdims=True))
    return (attended, source_grad, logits_grad)


def solution(mesh):
    torus = Mesh(mesh.devices.reshape(2, 2, 2, 4, 8), DP_MP)
    return jax.shard_map(
        on_device,
        mesh=torus,
        in_specs=(
            P(None, None, MP),
            P(),
            P(DP),
            P(None, MP),
            P(None, MP),
            P(DP_MP, None, None),
            P(DP_MP, None, None),
            P(DP_MP, None, None),
            P(DP_MP, None, None),
        ),
        out_specs=(P(DP_MP, None, None), P(None, DP, MP), P()),
        check_vma=False,
    )
```

```python
import jax
import jax.numpy as jnp
from jax import lax
from jax.experimental import pallas as pl
from jax.experimental.pallas import tpu as pltpu
from jax.sharding import Mesh
from jax.sharding import PartitionSpec as P

D = 4096
HEADS = 32
DH = 128
NSRC = 128
NTASK = 8
PTOK = 64
SEQ = 128
DP = ("dp_0", "dp_1")
MP = ("mp_0", "mp_1", "mp_2")
DP_MP = ("dp_0", "dp_1", "mp_0", "mp_1", "mp_2")
XY = ("mp_0", "mp_1")
XYC = ("dp_0", "dp_1", "mp_0", "mp_1")
GROUPS = 4
ROWS = PTOK // GROUPS
NXY = 8
NZ = 8
COLS = D // (NXY * NZ)
TROWS = NTASK * ROWS
SPAN = NZ * COLS
BF = jnp.bfloat16
F32 = jnp.float32


SMEM = pl.BlockSpec(memory_space=pltpu.SMEM)
VMEM = pl.BlockSpec(memory_space=pltpu.VMEM)


def dot(a, b, ca, cb):
    return lax.dot_general(a, b, (((ca,), (cb,)), ((), ())), preferred_element_type=F32)


def iota(shape, axis):
    return lax.broadcasted_iota(jnp.int32, shape, axis)


def lane_swap(a):
    return pltpu.roll(a, COLS, a.ndim - 1)


def lane_task(shape):
    return iota(shape, 1) % NTASK


def mixture_kernel(meta, logits_ref, prompts_ref, mix_ref, out_ref):
    logits = logits_ref[...]
    exponent = jnp.exp(logits - jnp.max(logits, axis=1, keepdims=True))
    mix = exponent / jnp.sum(exponent, axis=1, keepdims=True)
    mix_ref[...] = mix
    spread = (iota((NTASK, TROWS), 0) == lane_task((NTASK, TROWS))).astype(BF)
    by_lane = dot(mix.astype(BF), spread, 0, 0).astype(BF)
    rows = prompts_ref[...].reshape(ROWS * COLS, NSRC)
    every = dot(rows, by_lane, 1, 0)
    row = iota((COLS, TROWS), 1) // NTASK
    mixture = every[:COLS]
    for p in range(1, ROWS):
        mixture = jnp.where(row == p, every[p * COLS : (p + 1) * COLS], mixture)
    mixture = mixture.astype(BF)
    for k in range(NZ):
        out_ref[k] = mixture


def make_mixture(meta, logits, prompts):
    return pl.pallas_call(
        mixture_kernel,
        grid_spec=pltpu.PrefetchScalarGridSpec(
            num_scalar_prefetch=1,
            grid=(1,),
            in_specs=[
                pl.BlockSpec((NTASK, NSRC), lambda i, m: (0, 0)),
                pl.BlockSpec((ROWS, COLS, NSRC), lambda i, m: (m[0], 0, 0)),
            ],
            out_specs=[
                pl.BlockSpec((NTASK, NSRC), lambda i, m: (0, 0)),
                pl.BlockSpec((NZ, COLS, TROWS), lambda i, m: (0, 0, 0)),
            ],
        ),
        out_shape=[
            jax.ShapeDtypeStruct((NTASK, NSRC), F32),
            jax.ShapeDtypeStruct((NZ, COLS, TROWS), BF),
        ],
        name="mixture",
    )(meta, logits, prompts)


def task_major():
    r, c = iota((TROWS, TROWS), 0), iota((TROWS, TROWS), 1)
    return ((r % ROWS == c // NTASK) & (r // ROWS == c % NTASK)).astype(BF)


def project_kernel(meta, *refs):
    blocks, (key_ref, value_ref, out_ref) = refs[:NXY], refs[NXY:]
    total = jnp.zeros((2 * COLS, TROWS), F32)
    for k in range(NXY):
        start = pl.multiple_of((meta[1] ^ k) * SPAN, SPAN)
        weight = jnp.concatenate(
            [key_ref[:, pl.ds(start, SPAN)], value_ref[:, pl.ds(start, SPAN)]], axis=0
        )
        total += dot(weight, blocks[k][...], 1, 0)
    rows = dot(task_major(), total.astype(BF), 1, 1).astype(BF)
    for k in range(NZ):
        out_ref[k] = rows


def project(meta, blocks, key_weight, value_weight):
    return pl.pallas_call(
        project_kernel,
        in_specs=[SMEM] + [VMEM] * (NXY + 2),
        out_specs=VMEM,
        out_shape=jax.ShapeDtypeStruct((NZ, TROWS, 2 * COLS), BF),
        name="project",
    )(meta, *blocks, key_weight, value_weight)


def select_kernel(meta, i0, i1, i2, i3, in_ref, out_ref, table_ref):
    low = iota((NTASK, ROWS, 2 * COLS), 2) < COLS
    for h in range(NZ // 2):
        even = in_ref[2 * h].astype(F32)
        odd = in_ref[2 * h + 1].astype(F32)
        table_ref[:, h] = jnp.where(low, even, lane_swap(odd)).astype(BF)
        table_ref[:, NZ // 2 + h] = jnp.where(low, lane_swap(even), odd).astype(BF)
    group, z = meta[0], meta[2]
    for k, ids in enumerate((i0, i1, i2, i3)):
        for j in range(NXY):
            out_ref[(group ^ k) * NXY + j] = table_ref[ids[j * NZ + z]]


def select_prompts(meta, ids, gathered):
    return pl.pallas_call(
        select_kernel,
        in_specs=[SMEM] * 5 + [VMEM],
        out_specs=VMEM,
        out_shape=jax.ShapeDtypeStruct((GROUPS * NXY, NZ, ROWS, 2 * COLS), BF),
        scratch_shapes=[pltpu.VMEM((NTASK, NZ, ROWS, 2 * COLS), BF)],
    )(meta, *ids, gathered)


HEADS_AT_ONCE = 8
XY_AT_ONCE = HEADS_AT_ONCE * NXY // HEADS
SCALE = DH ** (-0.5)


def own_scores(k_ref, q_ref, at):
    visible = iota((SEQ, SEQ), 0) <= iota((SEQ, SEQ), 1)
    return jnp.where(visible, dot(k_ref[:, at], q_ref[:, at], 1, 1) * SCALE, -1e30)


def head_lanes():
    return [slice(h * DH, (h + 1) * DH) for h in range(HEADS_AT_ONCE)]


def prompt_part(prompt_ref, h, value):
    per = NZ // 2
    return prompt_ref[:, h // per, value * per + h % per].reshape(PTOK, DH)


def own_kernel(after_ref, q_ref, k_ref, v_ref, c_ref, stat_ref, s_ref, g_ref):
    del after_ref
    for h, at in enumerate(head_lanes()):
        s_ref[h] = own_scores(k_ref, q_ref, at)
        g_ref[h] = dot(v_ref[:, at], c_ref[:, at], 1, 1)
    for h in range(HEADS_AT_ONCE):
        scores = s_ref[h]
        top = jnp.max(scores, axis=0, keepdims=True)
        exponent = jnp.exp(scores - top)
        total = jnp.sum(exponent, axis=0, keepdims=True)
        inner = jnp.sum(exponent * g_ref[h], axis=0, keepdims=True)
        stat_ref[h] = jnp.concatenate([top, total, inner, jnp.zeros((5, SEQ), F32)], axis=0)


def grads_kernel(prompt_ref, stat_ref, q_ref, c_ref, grad_ref, norm_ref, s_ref, g_ref, p_ref, d_ref):
    for h, at in enumerate(head_lanes()):
        s_ref[h] = dot(prompt_part(prompt_ref, h, 0), q_ref[:, at], 1, 1) * SCALE
        g_ref[h] = dot(prompt_part(prompt_ref, h, 1), c_ref[:, at], 1, 1)
    for h in range(HEADS_AT_ONCE):
        own_top, own_total, own_inner = (stat_ref[h, i : i + 1] for i in range(3))
        scores, grads = s_ref[h], g_ref[h]
        top = jnp.maximum(jnp.max(scores, axis=0, keepdims=True), own_top)
        exponent = jnp.exp(scores - top)
        own = jnp.exp(own_top - top)
        share = 1.0 / (jnp.sum(exponent, axis=0, keepdims=True) + own * own_total)
        attn = exponent * share
        inner = jnp.sum(attn * grads, axis=0, keepdims=True) + own_inner * (own * share)
        p_ref[h] = attn.astype(BF)
        d_ref[h] = (attn * (grads - inner)).astype(BF)
        norm_ref[h] = jnp.concatenate([top, share, jnp.zeros((6, SEQ), F32)], axis=0)
    per = NZ // 2
    for h, at in enumerate(head_lanes()):
        kg = (dot(d_ref[h], q_ref[:, at], 1, 0) * SCALE).astype(BF)
        vg = dot(p_ref[h], c_ref[:, at], 1, 0).astype(BF)
        grad_ref[:, h // per, h % per] = kg.reshape(GROUPS, ROWS, DH)
        grad_ref[:, h // per, per + h % per] = vg.reshape(GROUPS, ROWS, DH)


def output_kernel(prompt_ref, norm_ref, q_ref, k_ref, v_ref, att_ref, s_ref, p_ref):
    for h, at in enumerate(head_lanes()):
        s_ref[h, :PTOK] = dot(prompt_part(prompt_ref, h, 0), q_ref[:, at], 1, 1) * SCALE
        s_ref[h, PTOK:] = own_scores(k_ref, q_ref, at)
    for h in range(HEADS_AT_ONCE):
        top, share = norm_ref[h, 0:1], norm_ref[h, 1:2]
        p_ref[h] = (jnp.exp(s_ref[h] - top) * share).astype(BF)
    for h, at in enumerate(head_lanes()):
        att = dot(p_ref[h, :PTOK], prompt_part(prompt_ref, h, 1), 0, 0)
        att += dot(p_ref[h, PTOK:], v_ref[:, at], 0, 0)
        att_ref[:, at] = att.astype(BF)


def attention_specs():
    seq = pl.BlockSpec((None, SEQ, DH * HEADS_AT_ONCE), lambda i: (0, 0, i))
    pair = pl.BlockSpec((GROUPS, XY_AT_ONCE, NZ, ROWS, DH), lambda i: (0, i, 0, 0, 0))
    stat = pl.BlockSpec((HEADS_AT_ONCE, 8, SEQ), lambda i: (i, 0, 0))
    return (HEADS // HEADS_AT_ONCE,), seq, pair, stat


def own_stats(after, queries, keys, values, cotangent):
    grid, seq, _, stat = attention_specs()
    square = pltpu.VMEM((HEADS_AT_ONCE, SEQ, SEQ), F32)
    return pl.pallas_call(
        own_kernel,
        grid=grid,
        in_specs=[pl.BlockSpec(memory_space=pl.ANY)] + [seq] * 4,
        out_specs=stat,
        out_shape=jax.ShapeDtypeStruct((HEADS, 8, SEQ), F32),
        scratch_shapes=[square, square],
        name="own_stats",
    )(after, queries, keys, values, cotangent)


def prompt_grads(prompts, stats, queries, cotangent):
    grid, seq, pair, stat = attention_specs()
    wide = (HEADS_AT_ONCE, PTOK, SEQ)
    return pl.pallas_call(
        grads_kernel,
        grid=grid,
        in_specs=[pair, stat, seq, seq],
        out_specs=[pair, stat],
        out_shape=[
            jax.ShapeDtypeStruct((GROUPS, NXY, NZ, ROWS, DH), BF),
            jax.ShapeDtypeStruct((HEADS, 8, SEQ), F32),
        ],
        scratch_shapes=[
            pltpu.VMEM(wide, F32),
            pltpu.VMEM(wide, F32),
            pltpu.VMEM(wide, BF),
            pltpu.VMEM(wide, BF),
        ],
        name="prompt_grads",
    )(prompts, stats, queries, cotangent)


def attention_output(prompts, norms, queries, keys, values):
    grid, seq, pair, stat = attention_specs()
    wide = (HEADS_AT_ONCE, PTOK + SEQ, SEQ)
    return pl.pallas_call(
        output_kernel,
        grid=grid,
        in_specs=[pair, stat, seq, seq, seq],
        out_specs=seq,
        out_shape=jax.ShapeDtypeStruct((1, SEQ, D), BF),
        scratch_shapes=[pltpu.VMEM(wide, F32), pltpu.VMEM(wide, BF)],
        name="attention_output",
    )(prompts, norms, queries, keys, values)


def tasks_kernel(meta, i0, i1, i2, i3, in_ref, after_ref, out_ref, total_ref):
    del after_ref
    total_ref[...] = jnp.zeros_like(total_ref)
    group, z = meta[0], meta[2]
    for k, ids in enumerate((i0, i1, i2, i3)):
        for j in range(NXY):
            total_ref[ids[j * NZ + z]] += in_ref[(group ^ k) * NXY + j].astype(F32)
    low = iota((NTASK, ROWS, 2 * COLS), 2) < COLS
    for h in range(NZ // 2):
        kg, vg = total_ref[:, h], total_ref[:, NZ // 2 + h]
        out_ref[2 * h] = jnp.where(low, kg, lane_swap(vg)).astype(BF)
        out_ref[2 * h + 1] = jnp.where(low, lane_swap(kg), vg).astype(BF)


def sum_by_task(meta, ids, incoming, after):
    return pl.pallas_call(
        tasks_kernel,
        in_specs=[SMEM] * 5 + [VMEM, pl.BlockSpec(memory_space=pl.ANY)],
        out_specs=VMEM,
        out_shape=jax.ShapeDtypeStruct((NZ, NTASK, ROWS, 2 * COLS), BF),
        scratch_shapes=[pltpu.VMEM((NTASK, NZ, ROWS, 2 * COLS), F32)],
    )(meta, *ids, incoming, after)


def halves(a):
    high = a.astype(BF)
    return high, (a - high.astype(F32)).astype(BF)


def rows_kernel(in_ref, key_ref, value_ref, out_ref):
    grads = in_ref[0].astype(F32)
    for k in range(1, NZ):
        grads += in_ref[k].astype(F32)
    order = task_major()
    left = jnp.concatenate([dot(order, part, 0, 0).astype(BF) for part in halves(grads)], axis=1)
    for k in range(NXY):
        at = slice(k * SPAN, (k + 1) * SPAN)
        keys, values = key_ref[:, at], value_ref[:, at]
        weight = jnp.concatenate([keys, values, keys, values], axis=0)
        out_ref[k] = dot(left, weight, 1, 0).astype(BF)


def row_terms(parts, key_weight, value_weight):
    return pl.pallas_call(
        rows_kernel,
        in_specs=[VMEM] * 3,
        out_specs=VMEM,
        out_shape=jax.ShapeDtypeStruct((NXY, TROWS, SPAN), BF),
        name="row_terms",
    )(parts, key_weight, value_weight)


def partial_kernel(in_ref, out_ref):
    total = in_ref[0].astype(F32)
    for k in range(1, NXY):
        total += in_ref[k].astype(F32)
    out_ref[...] = total.T.astype(BF).reshape(NZ, COLS, TROWS)


def partial_sums(terms):
    return pl.pallas_call(
        partial_kernel,
        in_specs=[VMEM],
        out_specs=VMEM,
        out_shape=jax.ShapeDtypeStruct((NZ, COLS, TROWS), BF),
        name="partial_sums",
    )(terms)


def weights_kernel(meta, in_ref, prompts_ref, tile_ref, weight_ref):
    tile = in_ref[0].astype(F32)
    for k in range(1, NZ):
        tile += in_ref[k].astype(F32)
    tile_ref[...] = tile
    turned = jnp.concatenate([tile, jnp.zeros_like(tile)], axis=0).T[:, :COLS]
    high, low = halves(turned)
    total = jnp.zeros((2 * NTASK, NSRC), F32)
    for p in range(ROWS):
        at = slice(p * NTASK, (p + 1) * NTASK)
        total += dot(jnp.concatenate([high[at], low[at]], axis=0), prompts_ref[p], 1, 0)
    weight_ref[...] = total[:NTASK] + total[NTASK:]


def weight_part(meta, parts, prompts):
    return pl.pallas_call(
        weights_kernel,
        grid_spec=pltpu.PrefetchScalarGridSpec(
            num_scalar_prefetch=1,
            grid=(1,),
            in_specs=[
                pl.BlockSpec((NZ, COLS, TROWS), lambda i, m: (0, 0, 0)),
                pl.BlockSpec((ROWS, COLS, NSRC), lambda i, m: (m[0], 0, 0)),
            ],
            out_specs=[
                pl.BlockSpec((COLS, TROWS), lambda i, m: (0, 0)),
                pl.BlockSpec((NTASK, NSRC), lambda i, m: (0, 0)),
            ],
        ),
        out_shape=[
            jax.ShapeDtypeStruct((COLS, TROWS), F32),
            jax.ShapeDtypeStruct((NTASK, NSRC), F32),
        ],
        name="weight_part",
    )(meta, parts, prompts)


def source_kernel(mix_ref, tile_ref, out_ref):
    spread = (iota((NTASK, TROWS), 0) == lane_task((NTASK, TROWS))).astype(BF)
    mix_high, mix_low = (dot(spread, m, 0, 0).astype(BF) for m in halves(mix_ref[...]))
    tile = tile_ref[...]
    row = iota((COLS, TROWS), 1) // NTASK
    for p in range(ROWS):
        high, low = halves(jnp.where(row == p, tile, 0.0))
        out_ref[p] = dot(high, mix_high, 1, 0) + dot(high, mix_low, 1, 0) + dot(low, mix_high, 1, 0)


def source_part(mix, tile):
    return pl.pallas_call(
        source_kernel,
        in_specs=[VMEM, VMEM],
        out_specs=VMEM,
        out_shape=jax.ShapeDtypeStruct((ROWS, COLS, NSRC), F32),
        name="source_part",
    )(mix, tile)


def exchange(blocks, axes):
    return lax.all_to_all(blocks, axes, split_axis=0, concat_axis=0, tiled=True)


def from_peers(array, axes, members):
    got = [array]
    for k in range(1, members):
        got.append(lax.ppermute(array, axes, [(i, i ^ k) for i in range(members)]))
    return got


def on_device(
    source_prompts,
    task_logits,
    task_ids,
    key_weight,
    value_weight,
    queries,
    keys,
    values,
    cotangent,
):
    meta = jnp.stack([lax.axis_index(DP), lax.axis_index(XY), lax.axis_index("mp_2")])
    meta = meta.astype(jnp.int32)
    prompts_in = source_prompts.transpose(1, 2, 0)
    key_in, value_in = key_weight.T, value_weight.T
    mix, copies = make_mixture(meta, task_logits, prompts_in)
    span = exchange(copies, "mp_2").reshape(SPAN, TROWS)
    span, task_ids = lax.optimization_barrier((span, task_ids))
    blocks = from_peers(span, XY, NXY)
    ids = from_peers(task_ids, DP, GROUPS)
    blocks, ids = lax.optimization_barrier((blocks, ids))
    copies = project(meta, blocks, key_in, value_in)
    gathered = exchange(copies, "mp_2").reshape(NZ, NTASK, ROWS, 2 * COLS)
    outgoing = select_prompts(meta, ids, gathered)
    stats = own_stats(outgoing, queries, keys, values, cotangent)
    prompts = exchange(outgoing, XYC).reshape(GROUPS, NXY, NZ, ROWS, DH)
    grads, norms = prompt_grads(prompts, stats, queries, cotangent)
    incoming = exchange(grads.reshape(GROUPS * NXY, NZ, ROWS, DH), XYC)
    attended = attention_output(prompts, norms, queries, keys, values)
    by_task = sum_by_task(meta, ids, incoming, attended).reshape(NZ, TROWS, 2 * COLS)
    parts = exchange(by_task, "mp_2")
    terms = exchange(row_terms(parts, key_in, value_in), XY)
    terms = exchange(partial_sums(terms), "mp_2")
    tile, weight_grad = weight_part(meta, terms, prompts_in)
    spread = jnp.broadcast_to(weight_grad[None], (GROUPS * NXY, NTASK, NSRC))
    weight_grad = exchange(spread, XYC).sum(axis=0)
    spread = jnp.broadcast_to(weight_grad[None], (NZ, NTASK, NSRC))
    weight_grad = exchange(spread, "mp_2").sum(axis=0)
    source_grad = source_part(mix, tile).transpose(2, 0, 1)
    logits_grad = mix * (weight_grad - jnp.sum(mix * weight_grad, axis=1, keepdims=True))
    return (attended, source_grad, logits_grad)


def solution(mesh):
    torus = Mesh(mesh.devices.reshape(2, 2, 2, 4, 8), DP_MP)
    return jax.shard_map(
        on_device,
        mesh=torus,
        in_specs=(
            P(None, None, MP),
            P(),
            P(DP),
            P(None, MP),
            P(None, MP),
            P(DP_MP, None, None),
            P(DP_MP, None, None),
            P(DP_MP, None, None),
            P(DP_MP, None, None),
        ),
        out_specs=(P(DP_MP, None, None), P(None, DP, MP), P()),
        check_vma=False,
    )
```

```python
import jax
import jax.numpy as jnp
from jax import lax
from jax.experimental import pallas as pl
from jax.experimental.pallas import tpu as pltpu
from jax.sharding import Mesh
from jax.sharding import PartitionSpec as P

D = 4096
HEADS = 32
DH = 128
NSRC = 128
NTASK = 8
PTOK = 64
SEQ = 128
DP = ("dp_0", "dp_1")
MP = ("mp_0", "mp_1", "mp_2")
DP_MP = ("dp_0", "dp_1", "mp_0", "mp_1", "mp_2")
XY = ("mp_0", "mp_1")
XYC = ("dp_0", "dp_1", "mp_0", "mp_1")
GROUPS = 4
ROWS = PTOK // GROUPS
NXY = 8
NZ = 8
COLS = D // (NXY * NZ)
TROWS = NTASK * ROWS
SPAN = NZ * COLS
BF = jnp.bfloat16
F32 = jnp.float32


SMEM = pl.BlockSpec(memory_space=pltpu.SMEM)
VMEM = pl.BlockSpec(memory_space=pltpu.VMEM)
ANY = pl.BlockSpec(memory_space=pl.ANY)


def dot(a, b, ca, cb):
    return lax.dot_general(a, b, (((ca,), (cb,)), ((), ())), preferred_element_type=F32)


def iota(shape, axis):
    return lax.broadcasted_iota(jnp.int32, shape, axis)


def lane_swap(a):
    return pltpu.roll(a, COLS, a.ndim - 1)


def lane_task(shape):
    return iota(shape, 1) % NTASK


def mixture_kernel(meta, logits_ref, prompts_ref, mix_ref, out_ref, rows_ref):
    rows_ref[...] = prompts_ref[...]
    logits = logits_ref[...]
    exponent = jnp.exp(logits - jnp.max(logits, axis=1, keepdims=True))
    mix = exponent / jnp.sum(exponent, axis=1, keepdims=True)
    mix_ref[...] = mix
    spread = (iota((NTASK, TROWS), 0) == lane_task((NTASK, TROWS))).astype(BF)
    by_lane = dot(mix.astype(BF), spread, 0, 0).astype(BF)
    rows = prompts_ref[...].reshape(ROWS * COLS, NSRC)
    every = dot(rows, by_lane, 1, 0)
    row = iota((COLS, TROWS), 1) // NTASK
    mixture = every[:COLS]
    for p in range(1, ROWS):
        mixture = jnp.where(row == p, every[p * COLS : (p + 1) * COLS], mixture)
    mixture = mixture.astype(BF)
    for k in range(NZ):
        out_ref[k] = mixture


def make_mixture(meta, logits, prompts):
    return pl.pallas_call(
        mixture_kernel,
        grid_spec=pltpu.PrefetchScalarGridSpec(
            num_scalar_prefetch=1,
            grid=(1,),
            in_specs=[
                pl.BlockSpec((NTASK, NSRC), lambda i, m: (0, 0)),
                pl.BlockSpec((ROWS, COLS, NSRC), lambda i, m: (m[0], 0, 0)),
            ],
            out_specs=[
                pl.BlockSpec((NTASK, NSRC), lambda i, m: (0, 0)),
                pl.BlockSpec((NZ, COLS, TROWS), lambda i, m: (0, 0, 0)),
                pl.BlockSpec((ROWS, COLS, NSRC), lambda i, m: (0, 0, 0)),
            ],
        ),
        out_shape=[
            jax.ShapeDtypeStruct((NTASK, NSRC), F32),
            jax.ShapeDtypeStruct((NZ, COLS, TROWS), BF),
            jax.ShapeDtypeStruct((ROWS, COLS, NSRC), BF),
        ],
        name="mixture",
    )(meta, logits, prompts)


def task_major():
    r, c = iota((TROWS, TROWS), 0), iota((TROWS, TROWS), 1)
    return ((r % ROWS == c // NTASK) & (r // ROWS == c % NTASK)).astype(BF)


def project_kernel(meta, *refs):
    blocks, (key_ref, value_ref, out_ref) = refs[:NXY], refs[NXY + 2 :]
    total = jnp.zeros((2 * COLS, TROWS), F32)
    for k in range(NXY):
        start = pl.multiple_of((meta[1] ^ k) * SPAN, SPAN)
        weight = jnp.concatenate(
            [key_ref[:, pl.ds(start, SPAN)], value_ref[:, pl.ds(start, SPAN)]], axis=0
        )
        total += dot(weight, blocks[k][...], 1, 0)
    rows = dot(task_major(), total.astype(BF), 1, 1).astype(BF)
    for k in range(NZ):
        out_ref[k] = rows


def project(meta, blocks, key_weight, value_weight, after):
    return pl.pallas_call(
        project_kernel,
        in_specs=[SMEM] + [VMEM] * NXY + [ANY] * 2 + [VMEM] * 2,
        out_specs=VMEM,
        out_shape=jax.ShapeDtypeStruct((NZ, TROWS, 2 * COLS), BF),
        name="project",
    )(meta, *blocks, *after, key_weight, value_weight)


def select_kernel(meta, i0, i1, i2, i3, in_ref, out_ref, table_ref):
    low = iota((NTASK, ROWS, 2 * COLS), 2) < COLS
    for h in range(NZ // 2):
        even = in_ref[2 * h].astype(F32)
        odd = in_ref[2 * h + 1].astype(F32)
        table_ref[:, h] = jnp.where(low, even, lane_swap(odd)).astype(BF)
        table_ref[:, NZ // 2 + h] = jnp.where(low, lane_swap(even), odd).astype(BF)
    group, z = meta[0], meta[2]
    for k, ids in enumerate((i0, i1, i2, i3)):
        for j in range(NXY):
            out_ref[(group ^ k) * NXY + j] = table_ref[ids[j * NZ + z]]


def select_prompts(meta, ids, gathered):
    return pl.pallas_call(
        select_kernel,
        in_specs=[SMEM] * 5 + [VMEM],
        out_specs=VMEM,
        out_shape=jax.ShapeDtypeStruct((GROUPS * NXY, NZ, ROWS, 2 * COLS), BF),
        scratch_shapes=[pltpu.VMEM((NTASK, NZ, ROWS, 2 * COLS), BF)],
    )(meta, *ids, gathered)


HEADS_AT_ONCE = 8
XY_AT_ONCE = HEADS_AT_ONCE * NXY // HEADS
SCALE = DH ** (-0.5)


def own_scores(k_ref, q_ref, at):
    visible = iota((SEQ, SEQ), 0) <= iota((SEQ, SEQ), 1)
    return jnp.where(visible, dot(k_ref[:, at], q_ref[:, at], 1, 1) * SCALE, -1e30)


def head_lanes():
    return [slice(h * DH, (h + 1) * DH) for h in range(HEADS_AT_ONCE)]


def prompt_part(prompt_ref, h, value):
    per = NZ // 2
    return prompt_ref[:, h // per, value * per + h % per].reshape(PTOK, DH)


def own_kernel(after_ref, q_ref, k_ref, v_ref, c_ref, stat_ref, s_ref, g_ref):
    del after_ref
    for h, at in enumerate(head_lanes()):
        s_ref[h] = own_scores(k_ref, q_ref, at)
        g_ref[h] = dot(v_ref[:, at], c_ref[:, at], 1, 1)
    for h in range(HEADS_AT_ONCE):
        scores = s_ref[h]
        top = jnp.max(scores, axis=0, keepdims=True)
        exponent = jnp.exp(scores - top)
        total = jnp.sum(exponent, axis=0, keepdims=True)
        inner = jnp.sum(exponent * g_ref[h], axis=0, keepdims=True)
        stat_ref[h] = jnp.concatenate([top, total, inner, jnp.zeros((5, SEQ), F32)], axis=0)


def grads_kernel(
    after0, after1, prompt_ref, stat_ref, q_ref, c_ref, grad_ref, norm_ref, s_ref, g_ref, p_ref, d_ref
):
    del after0, after1
    for h, at in enumerate(head_lanes()):
        s_ref[h] = dot(prompt_part(prompt_ref, h, 0), q_ref[:, at], 1, 1) * SCALE
        g_ref[h] = dot(prompt_part(prompt_ref, h, 1), c_ref[:, at], 1, 1)
    for h in range(HEADS_AT_ONCE):
        own_top, own_total, own_inner = (stat_ref[h, i : i + 1] for i in range(3))
        scores, grads = s_ref[h], g_ref[h]
        top = jnp.maximum(jnp.max(scores, axis=0, keepdims=True), own_top)
        exponent = jnp.exp(scores - top)
        own = jnp.exp(own_top - top)
        share = 1.0 / (jnp.sum(exponent, axis=0, keepdims=True) + own * own_total)
        attn = exponent * share
        inner = jnp.sum(attn * grads, axis=0, keepdims=True) + own_inner * (own * share)
        p_ref[h] = attn.astype(BF)
        d_ref[h] = (attn * (grads - inner)).astype(BF)
        norm_ref[h] = jnp.concatenate([top, share, jnp.zeros((6, SEQ), F32)], axis=0)
    per = NZ // 2
    for h, at in enumerate(head_lanes()):
        kg = (dot(d_ref[h], q_ref[:, at], 1, 0) * SCALE).astype(BF)
        vg = dot(p_ref[h], c_ref[:, at], 1, 0).astype(BF)
        grad_ref[:, h // per, h % per] = kg.reshape(GROUPS, ROWS, DH)
        grad_ref[:, h // per, per + h % per] = vg.reshape(GROUPS, ROWS, DH)


def output_kernel(prompt_ref, norm_ref, q_ref, k_ref, v_ref, att_ref, s_ref, p_ref):
    for h, at in enumerate(head_lanes()):
        s_ref[h, :PTOK] = dot(prompt_part(prompt_ref, h, 0), q_ref[:, at], 1, 1) * SCALE
        s_ref[h, PTOK:] = own_scores(k_ref, q_ref, at)
    for h in range(HEADS_AT_ONCE):
        top, share = norm_ref[h, 0:1], norm_ref[h, 1:2]
        p_ref[h] = (jnp.exp(s_ref[h] - top) * share).astype(BF)
    for h, at in enumerate(head_lanes()):
        att = dot(p_ref[h, :PTOK], prompt_part(prompt_ref, h, 1), 0, 0)
        att += dot(p_ref[h, PTOK:], v_ref[:, at], 0, 0)
        att_ref[:, at] = att.astype(BF)


def attention_specs():
    seq = pl.BlockSpec((None, SEQ, DH * HEADS_AT_ONCE), lambda i: (0, 0, i))
    pair = pl.BlockSpec((GROUPS, XY_AT_ONCE, NZ, ROWS, DH), lambda i: (0, i, 0, 0, 0))
    stat = pl.BlockSpec((HEADS_AT_ONCE, 8, SEQ), lambda i: (i, 0, 0))
    return (HEADS // HEADS_AT_ONCE,), seq, pair, stat


def own_stats(after, queries, keys, values, cotangent):
    grid, seq, _, stat = attention_specs()
    square = pltpu.VMEM((HEADS_AT_ONCE, SEQ, SEQ), F32)
    return pl.pallas_call(
        own_kernel,
        grid=grid,
        in_specs=[ANY] + [seq] * 4,
        out_specs=stat,
        out_shape=jax.ShapeDtypeStruct((HEADS, 8, SEQ), F32),
        scratch_shapes=[square, square],
        name="own_stats",
    )(after, queries, keys, values, cotangent)


def prompt_grads(after, prompts, stats, queries, cotangent):
    grid, seq, pair, stat = attention_specs()
    wide = (HEADS_AT_ONCE, PTOK, SEQ)
    return pl.pallas_call(
        grads_kernel,
        grid=grid,
        in_specs=[ANY, ANY, pair, stat, seq, seq],
        out_specs=[pair, stat],
        out_shape=[
            jax.ShapeDtypeStruct((GROUPS, NXY, NZ, ROWS, DH), BF),
            jax.ShapeDtypeStruct((HEADS, 8, SEQ), F32),
        ],
        scratch_shapes=[
            pltpu.VMEM(wide, F32),
            pltpu.VMEM(wide, F32),
            pltpu.VMEM(wide, BF),
            pltpu.VMEM(wide, BF),
        ],
        name="prompt_grads",
    )(*after, prompts, stats, queries, cotangent)


def attention_output(prompts, norms, queries, keys, values):
    grid, seq, pair, stat = attention_specs()
    wide = (HEADS_AT_ONCE, PTOK + SEQ, SEQ)
    return pl.pallas_call(
        output_kernel,
        grid=grid,
        in_specs=[pair, stat, seq, seq, seq],
        out_specs=seq,
        out_shape=jax.ShapeDtypeStruct((1, SEQ, D), BF),
        scratch_shapes=[pltpu.VMEM(wide, F32), pltpu.VMEM(wide, BF)],
        name="attention_output",
    )(prompts, norms, queries, keys, values)


def tasks_kernel(meta, i0, i1, i2, i3, in_ref, after0, after1, after2, out_ref, total_ref):
    del after0, after1, after2
    total_ref[...] = jnp.zeros_like(total_ref)
    group, z = meta[0], meta[2]
    for k, ids in enumerate((i0, i1, i2, i3)):
        for j in range(NXY):
            total_ref[ids[j * NZ + z]] += in_ref[(group ^ k) * NXY + j].astype(F32)
    low = iota((NTASK, ROWS, 2 * COLS), 2) < COLS
    for h in range(NZ // 2):
        kg, vg = total_ref[:, h], total_ref[:, NZ // 2 + h]
        out_ref[2 * h] = jnp.where(low, kg, lane_swap(vg)).astype(BF)
        out_ref[2 * h + 1] = jnp.where(low, lane_swap(kg), vg).astype(BF)


def sum_by_task(meta, ids, incoming, after):
    return pl.pallas_call(
        tasks_kernel,
        in_specs=[SMEM] * 5 + [VMEM] + [ANY] * 3,
        out_specs=VMEM,
        out_shape=jax.ShapeDtypeStruct((NZ, NTASK, ROWS, 2 * COLS), BF),
        scratch_shapes=[pltpu.VMEM((NTASK, NZ, ROWS, 2 * COLS), F32)],
    )(meta, *ids, incoming, *after)


def halves(a):
    high = a.astype(BF)
    return high, (a - high.astype(F32)).astype(BF)


def rows_kernel(in_ref, key_ref, value_ref, out_ref):
    grads = in_ref[0].astype(F32)
    for k in range(1, NZ):
        grads += in_ref[k].astype(F32)
    order = task_major()
    left = jnp.concatenate([dot(order, part, 0, 0).astype(BF) for part in halves(grads)], axis=1)
    for k in range(NXY):
        at = slice(k * SPAN, (k + 1) * SPAN)
        keys, values = key_ref[:, at], value_ref[:, at]
        weight = jnp.concatenate([keys, values, keys, values], axis=0)
        out_ref[k] = dot(left, weight, 1, 0).astype(BF)


def row_terms(parts, key_weight, value_weight):
    return pl.pallas_call(
        rows_kernel,
        in_specs=[VMEM] * 3,
        out_specs=VMEM,
        out_shape=jax.ShapeDtypeStruct((NXY, TROWS, SPAN), BF),
        name="row_terms",
    )(parts, key_weight, value_weight)


WBLOCK = COLS + 4 * NTASK
PAIRS = 2 * NTASK


def partial_kernel(meta, in_ref, *refs):
    prompts, (out_ref, part_ref) = refs[:NZ], refs[NZ:]
    total = in_ref[0].astype(F32)
    for k in range(1, NXY):
        total += in_ref[k].astype(F32)
    out_ref[:, :COLS] = total.T.astype(BF).reshape(NZ, COLS, TROWS)
    low = iota((TROWS, 2 * COLS), 1) < COLS
    for k in range(NZ // 2):
        pair = total[:, 2 * COLS * k : 2 * COLS * (k + 1)]
        part_ref[2 * k] = jnp.where(low, pair, 0.0)
        part_ref[2 * k + 1] = jnp.where(low, lane_swap(pair), 0.0)
    shift = [0, NZ - 1, 1, NZ - 2, 2, NZ - 3, 3, NZ - 4]
    sums = jnp.zeros((2 * PAIRS, 2 * NSRC), F32)
    for first in range(0, NZ, 4):
        parts = [part_ref[lax.rem(meta[2] + shift[k], NZ)] for k in range(first, first + 4)]
        left = jnp.concatenate([parts[k] + lane_swap(parts[k + 1]) for k in (0, 2)], axis=1)
        high, rest = halves(left)
        for p in range(0, ROWS, 2):
            at = slice(p * NTASK, p * NTASK + PAIRS)
            rows = jnp.concatenate([high[at], rest[at]], axis=0)
            columns = [
                jnp.concatenate([prompts[k][p + i] for k in range(first, first + 4)], axis=0)
                for i in range(2)
            ]
            sums += dot(rows, jnp.concatenate(columns, axis=1), 1, 0)
    weight = sums[:NTASK, :NSRC] + sums[NTASK:PAIRS, NSRC:]
    weight += sums[PAIRS : PAIRS + NTASK, :NSRC] + sums[PAIRS + NTASK :, NSRC:]
    high = weight.astype(BF).astype(F32)
    middle = (weight - high).astype(BF).astype(F32)
    terms = [high, middle, weight - high - middle, jnp.zeros_like(weight)]
    terms = jnp.concatenate(terms, axis=0).astype(BF)
    for k in range(NZ):
        out_ref[k, COLS:] = terms


def partial_sums(meta, terms, prompts):
    return pl.pallas_call(
        partial_kernel,
        in_specs=[SMEM] + [VMEM] * (1 + NZ),
        out_specs=VMEM,
        out_shape=jax.ShapeDtypeStruct((NZ, WBLOCK, TROWS), BF),
        scratch_shapes=[pltpu.VMEM((NZ, TROWS, 2 * COLS), F32)],
        name="partial_sums",
    )(meta, terms, *prompts)


def tile_kernel(in_ref, tile_ref, weight_ref):
    total = in_ref[0].astype(F32)
    for k in range(1, NZ):
        total += in_ref[k].astype(F32)
    tile_ref[...] = total[:COLS]
    high, middle, low = (total[COLS + k * NTASK : COLS + (k + 1) * NTASK] for k in range(3))
    weight = high + (middle + low)
    for k in range(GROUPS * NXY):
        weight_ref[k] = weight


def tile_sums(parts):
    return pl.pallas_call(
        tile_kernel,
        in_specs=[VMEM],
        out_specs=[VMEM, VMEM],
        out_shape=[
            jax.ShapeDtypeStruct((COLS, TROWS), F32),
            jax.ShapeDtypeStruct((GROUPS * NXY, NTASK, NSRC), F32),
        ],
        name="tile_sums",
    )(parts)


def source_kernel(mix_ref, tile_ref, out_ref):
    spread = (iota((NTASK, TROWS), 0) == lane_task((NTASK, TROWS))).astype(BF)
    mix_high, mix_low = (dot(spread, m, 0, 0).astype(BF) for m in halves(mix_ref[...]))
    tile = tile_ref[...]
    row = iota((COLS, TROWS), 1) // NTASK
    for p in range(ROWS):
        high, low = halves(jnp.where(row == p, tile, 0.0))
        out_ref[p] = dot(high, mix_high, 1, 0) + dot(high, mix_low, 1, 0) + dot(low, mix_high, 1, 0)


def source_part(mix, tile):
    return pl.pallas_call(
        source_kernel,
        in_specs=[VMEM, VMEM],
        out_specs=VMEM,
        out_shape=jax.ShapeDtypeStruct((ROWS, COLS, NSRC), F32),
        name="source_part",
    )(mix, tile)


def exchange(blocks, axes):
    return lax.all_to_all(blocks, axes, split_axis=0, concat_axis=0, tiled=True)


def from_peers(array, axes, members):
    got = [array]
    for k in range(1, members):
        got.append(lax.ppermute(array, axes, [(i, i ^ k) for i in range(members)]))
    return got


def ring_step(array, step):
    return lax.ppermute(array, "mp_2", [(i, (i + step) % NZ) for i in range(NZ)])


def on_device(
    source_prompts,
    task_logits,
    task_ids,
    key_weight,
    value_weight,
    queries,
    keys,
    values,
    cotangent,
):
    meta = jnp.stack([lax.axis_index(DP), lax.axis_index(XY), lax.axis_index("mp_2")])
    meta = meta.astype(jnp.int32)
    prompts_in = source_prompts.transpose(1, 2, 0)
    key_in, value_in = key_weight.T, value_weight.T
    mix, copies, rows = make_mixture(meta, task_logits, prompts_in)
    span = exchange(copies, "mp_2").reshape(SPAN, TROWS)
    blocks = from_peers(span, XY, NXY)
    around = [ring_step(rows, 1), ring_step(rows, -1)]
    copies = project(meta, blocks, key_in, value_in, around[:2])
    copies, task_ids = lax.optimization_barrier((copies, task_ids))
    ids = from_peers(task_ids, DP, GROUPS)
    gathered = exchange(copies, "mp_2").reshape(NZ, NTASK, ROWS, 2 * COLS)
    outgoing = select_prompts(meta, ids, gathered)
    stats = own_stats(outgoing, queries, keys, values, cotangent)
    around += [ring_step(around[0], 1), ring_step(around[1], -1)]
    prompts = exchange(outgoing, XYC).reshape(GROUPS, NXY, NZ, ROWS, DH)
    grads, norms = prompt_grads(around[2:4], prompts, stats, queries, cotangent)
    around += [ring_step(around[2], 1), ring_step(around[3], -1)]
    incoming = exchange(grads.reshape(GROUPS * NXY, NZ, ROWS, DH), XYC)
    attended = attention_output(prompts, norms, queries, keys, values)
    by_task = sum_by_task(meta, ids, incoming, [attended, *around[4:6]])
    around += [ring_step(around[4], 1)]
    parts = exchange(by_task.reshape(NZ, TROWS, 2 * COLS), "mp_2")
    terms = exchange(row_terms(parts, key_in, value_in), XY)
    terms = exchange(partial_sums(meta, terms, [rows, *around]), "mp_2")
    tile, spread = tile_sums(terms)
    weight_grad = exchange(spread, XYC).sum(axis=0)
    source_grad = source_part(mix, tile).transpose(2, 0, 1)
    logits_grad = mix * (weight_grad - jnp.sum(mix * weight_grad, axis=1, keepdims=True))
    return (attended, source_grad, logits_grad)


def solution(mesh):
    torus = Mesh(mesh.devices.reshape(2, 2, 2, 4, 8), DP_MP)
    return jax.shard_map(
        on_device,
        mesh=torus,
        in_specs=(
            P(None, None, MP),
            P(),
            P(DP),
            P(None, MP),
            P(None, MP),
            P(DP_MP, None, None),
            P(DP_MP, None, None),
            P(DP_MP, None, None),
            P(DP_MP, None, None),
        ),
        out_specs=(P(DP_MP, None, None), P(None, DP, MP), P()),
        check_vma=False,
    )
```

```python
import jax
import jax.numpy as jnp
from jax import lax
from jax.experimental import pallas as pl
from jax.experimental.pallas import tpu as pltpu
from jax.sharding import Mesh
from jax.sharding import PartitionSpec as P

D = 4096
HEADS = 32
DH = 128
NSRC = 128
NTASK = 8
PTOK = 64
SEQ = 128
DP = ("dp_0", "dp_1")
MP = ("mp_0", "mp_1", "mp_2")
DP_MP = ("dp_0", "dp_1", "mp_0", "mp_1", "mp_2")
XY = ("mp_0", "mp_1")
XYC = ("dp_0", "dp_1", "mp_0", "mp_1")
GROUPS = 4
ROWS = PTOK // GROUPS
NXY = 8
NZ = 8
COLS = D // (NXY * NZ)
TROWS = NTASK * ROWS
SPAN = NZ * COLS
BF = jnp.bfloat16
F32 = jnp.float32


SMEM = pl.BlockSpec(memory_space=pltpu.SMEM)
VMEM = pl.BlockSpec(memory_space=pltpu.VMEM)
ANY = pl.BlockSpec(memory_space=pl.ANY)


def dot(a, b, ca, cb):
    return lax.dot_general(a, b, (((ca,), (cb,)), ((), ())), preferred_element_type=F32)


def held(*arrays):
    kept = [pltpu.with_memory_space_constraint(a, pltpu.VMEM) for a in arrays]
    return kept if len(kept) > 1 else kept[0]


def in_hbm(*arrays):
    return [pltpu.with_memory_space_constraint(a, pltpu.HBM) for a in arrays]


def params(mib):
    return pltpu.CompilerParams(vmem_limit_bytes=mib * 2**20)


def iota(shape, axis):
    return lax.broadcasted_iota(jnp.int32, shape, axis)


def lane_swap(a):
    return pltpu.roll(a, COLS, a.ndim - 1)


def lane_task(shape):
    return iota(shape, 1) % NTASK


def mixture_kernel(meta, logits_ref, prompts_ref, mix_ref, out_ref, rows_ref):
    rows_ref[...] = prompts_ref[...]
    logits = logits_ref[...]
    exponent = jnp.exp(logits - jnp.max(logits, axis=1, keepdims=True))
    mix = exponent / jnp.sum(exponent, axis=1, keepdims=True)
    mix_ref[...] = mix
    spread = (iota((NTASK, TROWS), 0) == lane_task((NTASK, TROWS))).astype(BF)
    by_lane = dot(mix.astype(BF), spread, 0, 0).astype(BF)
    rows = prompts_ref[...].reshape(ROWS * COLS, NSRC)
    every = dot(rows, by_lane, 1, 0)
    row = iota((COLS, TROWS), 1) // NTASK
    mixture = every[:COLS]
    for p in range(1, ROWS):
        mixture = jnp.where(row == p, every[p * COLS : (p + 1) * COLS], mixture)
    mixture = mixture.astype(BF)
    for k in range(NZ):
        out_ref[k] = mixture


def make_mixture(meta, logits, prompts):
    return pl.pallas_call(
        mixture_kernel,
        grid_spec=pltpu.PrefetchScalarGridSpec(
            num_scalar_prefetch=1,
            grid=(1,),
            in_specs=[
                pl.BlockSpec((NTASK, NSRC), lambda i, m: (0, 0)),
                pl.BlockSpec((ROWS, COLS, NSRC), lambda i, m: (m[0], 0, 0)),
            ],
            out_specs=[
                pl.BlockSpec((NTASK, NSRC), lambda i, m: (0, 0)),
                pl.BlockSpec((NZ, COLS, TROWS), lambda i, m: (0, 0, 0)),
                pl.BlockSpec((ROWS, COLS, NSRC), lambda i, m: (0, 0, 0)),
            ],
        ),
        out_shape=[
            pltpu.VMEM((NTASK, NSRC), F32),
            jax.ShapeDtypeStruct((NZ, COLS, TROWS), BF),
            jax.ShapeDtypeStruct((ROWS, COLS, NSRC), BF),
        ],
        name="mixture",
        compiler_params=params(24),
    )(meta, *in_hbm(logits, prompts))


def task_major():
    r, c = iota((TROWS, TROWS), 0), iota((TROWS, TROWS), 1)
    return ((r % ROWS == c // NTASK) & (r // ROWS == c % NTASK)).astype(BF)


def project_kernel(meta, *refs):
    blocks, (key_ref, value_ref, out_ref) = refs[:NXY], refs[NXY + 2 :]
    total = jnp.zeros((2 * COLS, TROWS), F32)
    for k in range(NXY):
        start = pl.multiple_of((meta[1] ^ k) * SPAN, SPAN)
        weight = jnp.concatenate(
            [key_ref[:, pl.ds(start, SPAN)], value_ref[:, pl.ds(start, SPAN)]], axis=0
        )
        total += dot(weight, blocks[k][...], 1, 0)
    rows = dot(task_major(), total.astype(BF), 1, 1).astype(BF)
    for k in range(NZ):
        out_ref[k] = rows


def project(meta, blocks, key_weight, value_weight, after):
    return pl.pallas_call(
        project_kernel,
        in_specs=[SMEM] + [VMEM] * NXY + [ANY] * 2 + [VMEM] * 2,
        out_specs=VMEM,
        out_shape=jax.ShapeDtypeStruct((NZ, TROWS, 2 * COLS), BF),
        name="project",
        compiler_params=params(24),
    )(meta, *held(*blocks), *in_hbm(*after), *held(key_weight, value_weight))


def select_kernel(meta, i0, i1, i2, i3, in_ref, out_ref, table_ref):
    low = iota((NTASK, ROWS, 2 * COLS), 2) < COLS
    for h in range(NZ // 2):
        even = in_ref[2 * h].astype(F32)
        odd = in_ref[2 * h + 1].astype(F32)
        table_ref[:, h] = jnp.where(low, even, lane_swap(odd)).astype(BF)
        table_ref[:, NZ // 2 + h] = jnp.where(low, lane_swap(even), odd).astype(BF)
    group, z = meta[0], meta[2]
    for k, ids in enumerate((i0, i1, i2, i3)):
        for j in range(NXY):
            out_ref[(group ^ k) * NXY + j] = table_ref[ids[j * NZ + z]]


def select_prompts(meta, ids, gathered):
    return pl.pallas_call(
        select_kernel,
        in_specs=[SMEM] * 5 + [VMEM],
        out_specs=VMEM,
        out_shape=jax.ShapeDtypeStruct((GROUPS * NXY, NZ, ROWS, 2 * COLS), BF),
        scratch_shapes=[pltpu.VMEM((NTASK, NZ, ROWS, 2 * COLS), BF)],
        name="select",
        compiler_params=params(24),
    )(meta, *in_hbm(*ids), held(gathered))


HEADS_AT_ONCE = 8
XY_AT_ONCE = HEADS_AT_ONCE * NXY // HEADS
SCALE = DH ** (-0.5)


def own_scores(k_ref, q_ref, at):
    visible = iota((SEQ, SEQ), 0) <= iota((SEQ, SEQ), 1)
    return jnp.where(visible, dot(k_ref[:, at], q_ref[:, at], 1, 1) * SCALE, -1e30)


def head_lanes():
    return [slice(h * DH, (h + 1) * DH) for h in range(HEADS_AT_ONCE)]


def prompt_part(prompt_ref, h, value):
    per = NZ // 2
    at = pl.program_id(0) * XY_AT_ONCE + h // per
    return prompt_ref[:, at, value * per + h % per].reshape(PTOK, DH)


def own_kernel(after_ref, q_ref, k_ref, v_ref, c_ref, stat_ref, s_ref, g_ref):
    del after_ref
    for h, at in enumerate(head_lanes()):
        s_ref[h] = own_scores(k_ref, q_ref, at)
        g_ref[h] = dot(v_ref[:, at], c_ref[:, at], 1, 1)
    for h in range(HEADS_AT_ONCE):
        scores = s_ref[h]
        top = jnp.max(scores, axis=0, keepdims=True)
        exponent = jnp.exp(scores - top)
        total = jnp.sum(exponent, axis=0, keepdims=True)
        inner = jnp.sum(exponent * g_ref[h], axis=0, keepdims=True)
        stat_ref[h] = jnp.concatenate([top, total, inner, jnp.zeros((5, SEQ), F32)], axis=0)


def grads_kernel(
    after0, after1, prompt_ref, stat_ref, q_ref, c_ref, grad_ref, norm_ref, s_ref, g_ref, p_ref, d_ref
):
    del after0, after1
    for h, at in enumerate(head_lanes()):
        s_ref[h] = dot(prompt_part(prompt_ref, h, 0), q_ref[:, at], 1, 1) * SCALE
        g_ref[h] = dot(prompt_part(prompt_ref, h, 1), c_ref[:, at], 1, 1)
    for h in range(HEADS_AT_ONCE):
        own_top, own_total, own_inner = (stat_ref[h, i : i + 1] for i in range(3))
        scores, grads = s_ref[h], g_ref[h]
        top = jnp.maximum(jnp.max(scores, axis=0, keepdims=True), own_top)
        exponent = jnp.exp(scores - top)
        own = jnp.exp(own_top - top)
        share = 1.0 / (jnp.sum(exponent, axis=0, keepdims=True) + own * own_total)
        attn = exponent * share
        inner = jnp.sum(attn * grads, axis=0, keepdims=True) + own_inner * (own * share)
        p_ref[h] = attn.astype(BF)
        d_ref[h] = (attn * (grads - inner)).astype(BF)
        norm_ref[h] = jnp.concatenate([top, share, jnp.zeros((6, SEQ), F32)], axis=0)
    per = NZ // 2
    for h, at in enumerate(head_lanes()):
        kg = (dot(d_ref[h], q_ref[:, at], 1, 0) * SCALE).astype(BF)
        vg = dot(p_ref[h], c_ref[:, at], 1, 0).astype(BF)
        grad_ref[:, h // per, h % per] = kg.reshape(GROUPS, ROWS, DH)
        grad_ref[:, h // per, per + h % per] = vg.reshape(GROUPS, ROWS, DH)


def output_kernel(prompt_ref, norm_ref, q_ref, k_ref, v_ref, att_ref, s_ref, p_ref):
    for h, at in enumerate(head_lanes()):
        s_ref[h, :PTOK] = dot(prompt_part(prompt_ref, h, 0), q_ref[:, at], 1, 1) * SCALE
        s_ref[h, PTOK:] = own_scores(k_ref, q_ref, at)
    for h in range(HEADS_AT_ONCE):
        top, share = norm_ref[h, 0:1], norm_ref[h, 1:2]
        p_ref[h] = (jnp.exp(s_ref[h] - top) * share).astype(BF)
    for h, at in enumerate(head_lanes()):
        att = dot(p_ref[h, :PTOK], prompt_part(prompt_ref, h, 1), 0, 0)
        att += dot(p_ref[h, PTOK:], v_ref[:, at], 0, 0)
        att_ref[:, at] = att.astype(BF)


def attention_specs():
    seq = pl.BlockSpec((None, SEQ, DH * HEADS_AT_ONCE), lambda i: (0, 0, i))
    pair = pl.BlockSpec((GROUPS, XY_AT_ONCE, NZ, ROWS, DH), lambda i: (0, i, 0, 0, 0))
    stat = pl.BlockSpec((HEADS_AT_ONCE, 8, SEQ), lambda i: (i, 0, 0))
    return (HEADS // HEADS_AT_ONCE,), seq, pair, stat


def own_stats(after, queries, keys, values, cotangent):
    grid, seq, _, stat = attention_specs()
    square = pltpu.VMEM((HEADS_AT_ONCE, SEQ, SEQ), F32)
    return pl.pallas_call(
        own_kernel,
        grid=grid,
        in_specs=[ANY] + [seq] * 4,
        out_specs=stat,
        out_shape=jax.ShapeDtypeStruct((HEADS, 8, SEQ), F32),
        scratch_shapes=[square, square],
        name="own_stats",
        compiler_params=params(24),
    )(*in_hbm(after), queries, keys, values, cotangent)


def prompt_grads(after, prompts, stats, queries, cotangent):
    grid, seq, pair, stat = attention_specs()
    wide = (HEADS_AT_ONCE, PTOK, SEQ)
    return pl.pallas_call(
        grads_kernel,
        grid=grid,
        in_specs=[ANY, ANY, VMEM, stat, seq, seq],
        out_specs=[pair, stat],
        out_shape=[
            jax.ShapeDtypeStruct((GROUPS, NXY, NZ, ROWS, DH), BF),
            jax.ShapeDtypeStruct((HEADS, 8, SEQ), F32),
        ],
        scratch_shapes=[
            pltpu.VMEM(wide, F32),
            pltpu.VMEM(wide, F32),
            pltpu.VMEM(wide, BF),
            pltpu.VMEM(wide, BF),
        ],
        name="prompt_grads",
        compiler_params=params(24),
    )(*in_hbm(*after), held(prompts), stats, queries, cotangent)


def attention_output(prompts, norms, queries, keys, values):
    grid, seq, _, stat = attention_specs()
    wide = (HEADS_AT_ONCE, PTOK + SEQ, SEQ)
    return pl.pallas_call(
        output_kernel,
        grid=grid,
        in_specs=[VMEM, stat, seq, seq, seq],
        out_specs=seq,
        out_shape=jax.ShapeDtypeStruct((1, SEQ, D), BF),
        scratch_shapes=[pltpu.VMEM(wide, F32), pltpu.VMEM(wide, BF)],
        name="attention_output",
        compiler_params=params(24),
    )(held(prompts), norms, queries, keys, values)


def tasks_kernel(meta, i0, i1, i2, i3, in_ref, after0, after1, after2, out_ref, total_ref):
    del after0, after1, after2
    total_ref[...] = jnp.zeros_like(total_ref)
    group, z = meta[0], meta[2]
    for k, ids in enumerate((i0, i1, i2, i3)):
        for j in range(NXY):
            total_ref[ids[j * NZ + z]] += in_ref[(group ^ k) * NXY + j].astype(F32)
    low = iota((NTASK, ROWS, 2 * COLS), 2) < COLS
    for h in range(NZ // 2):
        kg, vg = total_ref[:, h], total_ref[:, NZ // 2 + h]
        out_ref[2 * h] = jnp.where(low, kg, lane_swap(vg)).astype(BF)
        out_ref[2 * h + 1] = jnp.where(low, lane_swap(kg), vg).astype(BF)


def sum_by_task(meta, ids, incoming, after):
    return pl.pallas_call(
        tasks_kernel,
        in_specs=[SMEM] * 5 + [VMEM] + [ANY] * 3,
        out_specs=VMEM,
        out_shape=jax.ShapeDtypeStruct((NZ, NTASK, ROWS, 2 * COLS), BF),
        scratch_shapes=[pltpu.VMEM((NTASK, NZ, ROWS, 2 * COLS), F32)],
        name="by_task",
        compiler_params=params(24),
    )(meta, *in_hbm(*ids), held(incoming), *in_hbm(*after))


def halves(a):
    high = a.astype(BF)
    return high, (a - high.astype(F32)).astype(BF)


def rows_kernel(in_ref, key_ref, value_ref, out_ref):
    grads = in_ref[0].astype(F32)
    for k in range(1, NZ):
        grads += in_ref[k].astype(F32)
    order = task_major()
    left = jnp.concatenate([dot(order, part, 0, 0).astype(BF) for part in halves(grads)], axis=1)
    for k in range(NXY):
        at = slice(k * SPAN, (k + 1) * SPAN)
        keys, values = key_ref[:, at], value_ref[:, at]
        weight = jnp.concatenate([keys, values, keys, values], axis=0)
        out_ref[k] = dot(left, weight, 1, 0).astype(BF)


def row_terms(parts, key_weight, value_weight):
    return pl.pallas_call(
        rows_kernel,
        in_specs=[VMEM] * 3,
        out_specs=VMEM,
        out_shape=jax.ShapeDtypeStruct((NXY, TROWS, SPAN), BF),
        name="row_terms",
        compiler_params=params(24),
    )(*held(parts, key_weight, value_weight))


WBLOCK = COLS + 4 * NTASK
PAIRS = 2 * NTASK


def partial_kernel(meta, in_ref, *refs):
    prompts, (out_ref, part_ref) = refs[:NZ], refs[NZ:]
    total = in_ref[0].astype(F32)
    for k in range(1, NXY):
        total += in_ref[k].astype(F32)
    out_ref[:, :COLS] = total.T.astype(BF).reshape(NZ, COLS, TROWS)
    low = iota((TROWS, 2 * COLS), 1) < COLS
    for k in range(NZ // 2):
        pair = total[:, 2 * COLS * k : 2 * COLS * (k + 1)]
        part_ref[2 * k] = jnp.where(low, pair, 0.0)
        part_ref[2 * k + 1] = jnp.where(low, lane_swap(pair), 0.0)
    shift = [0, NZ - 1, 1, NZ - 2, 2, NZ - 3, 3, NZ - 4]
    sums = jnp.zeros((2 * PAIRS, 2 * NSRC), F32)
    for first in range(0, NZ, 4):
        parts = [part_ref[lax.rem(meta[2] + shift[k], NZ)] for k in range(first, first + 4)]
        left = jnp.concatenate([parts[k] + lane_swap(parts[k + 1]) for k in (0, 2)], axis=1)
        high, rest = halves(left)
        for p in range(0, ROWS, 2):
            at = slice(p * NTASK, p * NTASK + PAIRS)
            rows = jnp.concatenate([high[at], rest[at]], axis=0)
            columns = [
                jnp.concatenate([prompts[k][p + i] for k in range(first, first + 4)], axis=0)
                for i in range(2)
            ]
            sums += dot(rows, jnp.concatenate(columns, axis=1), 1, 0)
    weight = sums[:NTASK, :NSRC] + sums[NTASK:PAIRS, NSRC:]
    weight += sums[PAIRS : PAIRS + NTASK, :NSRC] + sums[PAIRS + NTASK :, NSRC:]
    high = weight.astype(BF).astype(F32)
    middle = (weight - high).astype(BF).astype(F32)
    terms = [high, middle, weight - high - middle, jnp.zeros_like(weight)]
    terms = jnp.concatenate(terms, axis=0).astype(BF)
    for k in range(NZ):
        out_ref[k, COLS:] = terms


def partial_sums(meta, terms, prompts):
    return pl.pallas_call(
        partial_kernel,
        in_specs=[SMEM] + [VMEM] * (1 + NZ),
        out_specs=VMEM,
        out_shape=jax.ShapeDtypeStruct((NZ, WBLOCK, TROWS), BF),
        scratch_shapes=[pltpu.VMEM((NZ, TROWS, 2 * COLS), F32)],
        name="partial_sums",
        compiler_params=params(24),
    )(meta, *held(terms, *prompts))


def tile_kernel(in_ref, tile_ref, weight_ref):
    total = in_ref[0].astype(F32)
    for k in range(1, NZ):
        total += in_ref[k].astype(F32)
    tile_ref[...] = total[:COLS]
    high, middle, low = (total[COLS + k * NTASK : COLS + (k + 1) * NTASK] for k in range(3))
    weight = high + (middle + low)
    for k in range(GROUPS * NXY):
        weight_ref[k] = weight


def tile_sums(parts):
    return pl.pallas_call(
        tile_kernel,
        in_specs=[VMEM],
        out_specs=[VMEM, VMEM],
        out_shape=[
            pltpu.VMEM((COLS, TROWS), F32),
            jax.ShapeDtypeStruct((GROUPS * NXY, NTASK, NSRC), F32),
        ],
        name="tile_sums",
        compiler_params=params(24),
    )(held(parts))


def source_kernel(mix_ref, tile_ref, out_ref):
    spread = (iota((NTASK, TROWS), 0) == lane_task((NTASK, TROWS))).astype(BF)
    mix_high, mix_low = (dot(spread, m, 0, 0).astype(BF) for m in halves(mix_ref[...]))
    tile = tile_ref[...]
    row = iota((COLS, TROWS), 1) // NTASK
    for p in range(ROWS):
        high, low = halves(jnp.where(row == p, tile, 0.0))
        out_ref[p] = dot(high, mix_high, 1, 0) + dot(high, mix_low, 1, 0) + dot(low, mix_high, 1, 0)


def source_part(mix, tile):
    return pl.pallas_call(
        source_kernel,
        in_specs=[VMEM, VMEM],
        out_specs=VMEM,
        out_shape=jax.ShapeDtypeStruct((ROWS, COLS, NSRC), F32),
        name="source_part",
        compiler_params=params(24),
    )(*held(mix, tile))


def exchange(blocks, axes):
    return lax.all_to_all(blocks, axes, split_axis=0, concat_axis=0, tiled=True)


def from_peers(array, axes, members):
    got = [array]
    for k in range(1, members):
        got.append(lax.ppermute(array, axes, [(i, i ^ k) for i in range(members)]))
    return got


def ring_step(array, step):
    return lax.ppermute(array, "mp_2", [(i, (i + step) % NZ) for i in range(NZ)])


def on_device(
    source_prompts,
    task_logits,
    task_ids,
    key_weight,
    value_weight,
    queries,
    keys,
    values,
    cotangent,
):
    meta = jnp.stack([lax.axis_index(DP), lax.axis_index(XY), lax.axis_index("mp_2")])
    meta = meta.astype(jnp.int32)
    prompts_in = source_prompts.transpose(1, 2, 0)
    key_in, value_in = key_weight.T, value_weight.T
    mix, copies, rows = make_mixture(meta, task_logits, prompts_in)
    span = exchange(copies, "mp_2").reshape(SPAN, TROWS)
    blocks = from_peers(span, XY, NXY)
    around = [ring_step(rows, 1), ring_step(rows, -1)]
    copies = project(meta, blocks, key_in, value_in, around[:2])
    copies, task_ids = lax.optimization_barrier((copies, task_ids))
    ids = from_peers(task_ids, DP, GROUPS)
    gathered = exchange(copies, "mp_2").reshape(NZ, NTASK, ROWS, 2 * COLS)
    outgoing = select_prompts(meta, ids, gathered)
    stats = own_stats(outgoing, queries, keys, values, cotangent)
    around += [ring_step(around[0], 1), ring_step(around[1], -1)]
    prompts = exchange(outgoing, XYC).reshape(GROUPS, NXY, NZ, ROWS, DH)
    grads, norms = prompt_grads(around[2:4], prompts, stats, queries, cotangent)
    around += [ring_step(around[2], 1), ring_step(around[3], -1)]
    incoming = exchange(grads.reshape(GROUPS * NXY, NZ, ROWS, DH), XYC)
    attended = attention_output(prompts, norms, queries, keys, values)
    by_task = sum_by_task(meta, ids, incoming, [attended, *around[4:6]])
    around += [ring_step(around[4], 1)]
    parts = exchange(by_task.reshape(NZ, TROWS, 2 * COLS), "mp_2")
    terms = exchange(row_terms(parts, key_in, value_in), XY)
    terms = exchange(partial_sums(meta, terms, [rows, *around]), "mp_2")
    tile, spread = tile_sums(terms)
    weight_grad = exchange(spread, XYC).sum(axis=0)
    source_grad = source_part(mix, tile).transpose(2, 0, 1)
    logits_grad = mix * (weight_grad - jnp.sum(mix * weight_grad, axis=1, keepdims=True))
    return (attended, source_grad, logits_grad)


def solution(mesh):
    torus = Mesh(mesh.devices.reshape(2, 2, 2, 4, 8), DP_MP)
    return jax.shard_map(
        on_device,
        mesh=torus,
        in_specs=(
            P(None, None, MP),
            P(),
            P(DP),
            P(None, MP),
            P(None, MP),
            P(DP_MP, None, None),
            P(DP_MP, None, None),
            P(DP_MP, None, None),
            P(DP_MP, None, None),
        ),
        out_specs=(P(DP_MP, None, None), P(None, DP, MP), P()),
        check_vma=False,
    )
```

```python
import jax
import jax.numpy as jnp
from jax import lax
from jax.experimental import pallas as pl
from jax.experimental.pallas import tpu as pltpu
from jax.sharding import Mesh
from jax.sharding import PartitionSpec as P

D = 4096
HEADS = 32
DH = 128
NSRC = 128
NTASK = 8
PTOK = 64
SEQ = 128
DP = ("dp_0", "dp_1")
MP = ("mp_0", "mp_1", "mp_2")
DP_MP = ("dp_0", "dp_1", "mp_0", "mp_1", "mp_2")
XY = ("mp_0", "mp_1")
XYC = ("dp_0", "dp_1", "mp_0", "mp_1")
GROUPS = 4
ROWS = PTOK // GROUPS
NXY = 8
NZ = 8
COLS = D // (NXY * NZ)
TROWS = NTASK * ROWS
SPAN = NZ * COLS
BF = jnp.bfloat16
F32 = jnp.float32


SMEM = pl.BlockSpec(memory_space=pltpu.SMEM)
VMEM = pl.BlockSpec(memory_space=pltpu.VMEM)
ANY = pl.BlockSpec(memory_space=pl.ANY)


def dot(a, b, ca, cb):
    return lax.dot_general(a, b, (((ca,), (cb,)), ((), ())), preferred_element_type=F32)


def held(*arrays):
    kept = [pltpu.with_memory_space_constraint(a, pltpu.VMEM) for a in arrays]
    return kept if len(kept) > 1 else kept[0]


def in_hbm(*arrays):
    return [pltpu.with_memory_space_constraint(a, pltpu.HBM) for a in arrays]


def params(mib):
    return pltpu.CompilerParams(vmem_limit_bytes=mib * 2**20)


def iota(shape, axis):
    return lax.broadcasted_iota(jnp.int32, shape, axis)


def lane_swap(a):
    return pltpu.roll(a, COLS, a.ndim - 1)


def lane_task(shape):
    return iota(shape, 1) % NTASK


def mixture_kernel(meta, logits_ref, prompts_ref, mix_ref, out_ref, rows_ref):
    rows_ref[...] = prompts_ref[...]
    logits = logits_ref[...]
    exponent = jnp.exp(logits - jnp.max(logits, axis=1, keepdims=True))
    mix = exponent / jnp.sum(exponent, axis=1, keepdims=True)
    mix_ref[...] = mix
    spread = (iota((NTASK, TROWS), 0) == lane_task((NTASK, TROWS))).astype(BF)
    by_lane = dot(mix.astype(BF), spread, 0, 0).astype(BF)
    rows = prompts_ref[...].reshape(ROWS * COLS, NSRC)
    every = dot(rows, by_lane, 1, 0)
    row = iota((COLS, TROWS), 1) // NTASK
    mixture = every[:COLS]
    for p in range(1, ROWS):
        mixture = jnp.where(row == p, every[p * COLS : (p + 1) * COLS], mixture)
    mixture = mixture.astype(BF)
    for k in range(NZ):
        out_ref[k] = mixture


def make_mixture(meta, logits, prompts):
    return pl.pallas_call(
        mixture_kernel,
        grid_spec=pltpu.PrefetchScalarGridSpec(
            num_scalar_prefetch=1,
            grid=(1,),
            in_specs=[
                pl.BlockSpec((NTASK, NSRC), lambda i, m: (0, 0)),
                pl.BlockSpec((ROWS, COLS, NSRC), lambda i, m: (m[0], 0, 0)),
            ],
            out_specs=[
                pl.BlockSpec((NTASK, NSRC), lambda i, m: (0, 0)),
                pl.BlockSpec((NZ, COLS, TROWS), lambda i, m: (0, 0, 0)),
                pl.BlockSpec((ROWS, COLS, NSRC), lambda i, m: (0, 0, 0)),
            ],
        ),
        out_shape=[
            pltpu.VMEM((NTASK, NSRC), F32),
            jax.ShapeDtypeStruct((NZ, COLS, TROWS), BF),
            jax.ShapeDtypeStruct((ROWS, COLS, NSRC), BF),
        ],
        name="mixture",
        compiler_params=params(24),
    )(meta, *in_hbm(logits, prompts))


def task_major():
    r, c = iota((TROWS, TROWS), 0), iota((TROWS, TROWS), 1)
    return ((r % ROWS == c // NTASK) & (r // ROWS == c % NTASK)).astype(BF)


def project_kernel(meta, *refs):
    blocks, (key_ref, value_ref, out_ref) = refs[:NXY], refs[NXY + 2 :]
    total = jnp.zeros((2 * COLS, TROWS), F32)
    for k in range(NXY):
        start = pl.multiple_of((meta[1] ^ k) * SPAN, SPAN)
        weight = jnp.concatenate(
            [key_ref[:, pl.ds(start, SPAN)], value_ref[:, pl.ds(start, SPAN)]], axis=0
        )
        total += dot(weight, blocks[k][...], 1, 0)
    rows = dot(task_major(), total.astype(BF), 1, 1).astype(BF)
    for k in range(NZ):
        out_ref[k] = rows


def project(meta, blocks, key_weight, value_weight, after):
    return pl.pallas_call(
        project_kernel,
        in_specs=[SMEM] + [VMEM] * NXY + [ANY] * 2 + [VMEM] * 2,
        out_specs=VMEM,
        out_shape=jax.ShapeDtypeStruct((NZ, TROWS, 2 * COLS), BF),
        name="project",
        compiler_params=params(24),
    )(meta, *held(*blocks), *in_hbm(*after), *held(key_weight, value_weight))


def select_kernel(meta, i0, i1, i2, i3, in_ref, out_ref, table_ref):
    low = iota((NTASK, ROWS, 2 * COLS), 2) < COLS
    for h in range(NZ // 2):
        even = in_ref[2 * h].astype(F32)
        odd = in_ref[2 * h + 1].astype(F32)
        table_ref[:, h] = jnp.where(low, even, lane_swap(odd)).astype(BF)
        table_ref[:, NZ // 2 + h] = jnp.where(low, lane_swap(even), odd).astype(BF)
    group, z = meta[0], meta[2]
    for k, ids in enumerate((i0, i1, i2, i3)):
        for j in range(NXY):
            out_ref[(group ^ k) * NXY + j] = table_ref[ids[j * NZ + z]]


def select_prompts(meta, ids, gathered):
    return pl.pallas_call(
        select_kernel,
        in_specs=[SMEM] * 5 + [VMEM],
        out_specs=VMEM,
        out_shape=jax.ShapeDtypeStruct((GROUPS * NXY, NZ, ROWS, 2 * COLS), BF),
        scratch_shapes=[pltpu.VMEM((NTASK, NZ, ROWS, 2 * COLS), BF)],
        name="select",
        compiler_params=params(24),
    )(meta, *in_hbm(*ids), held(gathered))


HEADS_AT_ONCE = 8
XY_AT_ONCE = HEADS_AT_ONCE * NXY // HEADS
SCALE = DH ** (-0.5)


def own_scores(k_ref, q_ref, at):
    visible = iota((SEQ, SEQ), 0) <= iota((SEQ, SEQ), 1)
    return jnp.where(visible, dot(k_ref[:, at], q_ref[:, at], 1, 1) * SCALE, -1e30)


def head_lanes():
    return [slice(h * DH, (h + 1) * DH) for h in range(HEADS_AT_ONCE)]


def prompt_part(prompt_ref, h, value):
    per = NZ // 2
    at = pl.program_id(0) * XY_AT_ONCE + h // per
    return prompt_ref[:, at, value * per + h % per].reshape(PTOK, DH)


def own_kernel(after_ref, q_ref, k_ref, v_ref, c_ref, stat_ref, s_ref, g_ref):
    del after_ref
    for h, at in enumerate(head_lanes()):
        s_ref[h] = own_scores(k_ref, q_ref, at)
        g_ref[h] = dot(v_ref[:, at], c_ref[:, at], 1, 1)
    for h in range(HEADS_AT_ONCE):
        scores = s_ref[h]
        top = jnp.max(scores, axis=0, keepdims=True)
        exponent = jnp.exp(scores - top)
        total = jnp.sum(exponent, axis=0, keepdims=True)
        inner = jnp.sum(exponent * g_ref[h], axis=0, keepdims=True)
        stat_ref[h] = jnp.concatenate([top, total, inner, jnp.zeros((5, SEQ), F32)], axis=0)


def grads_kernel(
    after0, after1, prompt_ref, stat_ref, q_ref, c_ref, grad_ref, norm_ref, s_ref, g_ref, p_ref, d_ref
):
    del after0, after1
    for h, at in enumerate(head_lanes()):
        s_ref[h] = dot(prompt_part(prompt_ref, h, 0), q_ref[:, at], 1, 1) * SCALE
        g_ref[h] = dot(prompt_part(prompt_ref, h, 1), c_ref[:, at], 1, 1)
    for h in range(HEADS_AT_ONCE):
        own_top, own_total, own_inner = (stat_ref[h, i : i + 1] for i in range(3))
        scores, grads = s_ref[h], g_ref[h]
        top = jnp.maximum(jnp.max(scores, axis=0, keepdims=True), own_top)
        exponent = jnp.exp(scores - top)
        own = jnp.exp(own_top - top)
        share = 1.0 / (jnp.sum(exponent, axis=0, keepdims=True) + own * own_total)
        attn = exponent * share
        inner = jnp.sum(attn * grads, axis=0, keepdims=True) + own_inner * (own * share)
        p_ref[h] = attn.astype(BF)
        d_ref[h] = (attn * (grads - inner)).astype(BF)
        norm_ref[h] = jnp.concatenate([top, share, jnp.zeros((6, SEQ), F32)], axis=0)
    per = NZ // 2
    for h, at in enumerate(head_lanes()):
        kg = (dot(d_ref[h], q_ref[:, at], 1, 0) * SCALE).astype(BF)
        vg = dot(p_ref[h], c_ref[:, at], 1, 0).astype(BF)
        grad_ref[:, h // per, h % per] = kg.reshape(GROUPS, ROWS, DH)
        grad_ref[:, h // per, per + h % per] = vg.reshape(GROUPS, ROWS, DH)


def output_kernel(prompt_ref, norm_ref, q_ref, k_ref, v_ref, att_ref, s_ref, p_ref):
    for h, at in enumerate(head_lanes()):
        s_ref[h, :PTOK] = dot(prompt_part(prompt_ref, h, 0), q_ref[:, at], 1, 1) * SCALE
        s_ref[h, PTOK:] = own_scores(k_ref, q_ref, at)
    for h in range(HEADS_AT_ONCE):
        top, share = norm_ref[h, 0:1], norm_ref[h, 1:2]
        p_ref[h] = (jnp.exp(s_ref[h] - top) * share).astype(BF)
    for h, at in enumerate(head_lanes()):
        att = dot(p_ref[h, :PTOK], prompt_part(prompt_ref, h, 1), 0, 0)
        att += dot(p_ref[h, PTOK:], v_ref[:, at], 0, 0)
        att_ref[:, at] = att.astype(BF)


def attention_specs():
    seq = pl.BlockSpec((None, SEQ, DH * HEADS_AT_ONCE), lambda i: (0, 0, i))
    pair = pl.BlockSpec((GROUPS, XY_AT_ONCE, NZ, ROWS, DH), lambda i: (0, i, 0, 0, 0))
    stat = pl.BlockSpec((HEADS_AT_ONCE, 8, SEQ), lambda i: (i, 0, 0))
    return (HEADS // HEADS_AT_ONCE,), seq, pair, stat


def own_stats(after, queries, keys, values, cotangent):
    grid, seq, _, stat = attention_specs()
    square = pltpu.VMEM((HEADS_AT_ONCE, SEQ, SEQ), F32)
    return pl.pallas_call(
        own_kernel,
        grid=grid,
        in_specs=[ANY] + [seq] * 4,
        out_specs=stat,
        out_shape=jax.ShapeDtypeStruct((HEADS, 8, SEQ), F32),
        scratch_shapes=[square, square],
        name="own_stats",
        compiler_params=params(24),
    )(*in_hbm(after), queries, keys, values, cotangent)


def prompt_grads(after, prompts, stats, queries, cotangent):
    grid, seq, pair, stat = attention_specs()
    wide = (HEADS_AT_ONCE, PTOK, SEQ)
    return pl.pallas_call(
        grads_kernel,
        grid=grid,
        in_specs=[ANY, ANY, VMEM, stat, seq, seq],
        out_specs=[pair, stat],
        out_shape=[
            pltpu.HBM((GROUPS, NXY, NZ, ROWS, DH), BF),
            pltpu.HBM((HEADS, 8, SEQ), F32),
        ],
        scratch_shapes=[
            pltpu.VMEM(wide, F32),
            pltpu.VMEM(wide, F32),
            pltpu.VMEM(wide, BF),
            pltpu.VMEM(wide, BF),
        ],
        name="prompt_grads",
        compiler_params=params(24),
    )(*in_hbm(*after), held(prompts), stats, queries, cotangent)


def attention_output(prompts, norms, queries, keys, values):
    grid, seq, _, stat = attention_specs()
    wide = (HEADS_AT_ONCE, PTOK + SEQ, SEQ)
    return pl.pallas_call(
        output_kernel,
        grid=grid,
        in_specs=[VMEM, stat, seq, seq, seq],
        out_specs=seq,
        out_shape=jax.ShapeDtypeStruct((1, SEQ, D), BF),
        scratch_shapes=[pltpu.VMEM(wide, F32), pltpu.VMEM(wide, BF)],
        name="attention_output",
        compiler_params=params(24),
    )(held(prompts), norms, queries, keys, values)


def tasks_kernel(meta, i0, i1, i2, i3, in_ref, after0, after1, after2, out_ref, total_ref):
    del after0, after1, after2
    total_ref[...] = jnp.zeros_like(total_ref)
    group, z = meta[0], meta[2]
    for k, ids in enumerate((i0, i1, i2, i3)):
        for j in range(NXY):
            total_ref[ids[j * NZ + z]] += in_ref[(group ^ k) * NXY + j].astype(F32)
    low = iota((NTASK, ROWS, 2 * COLS), 2) < COLS
    for h in range(NZ // 2):
        kg, vg = total_ref[:, h], total_ref[:, NZ // 2 + h]
        out_ref[2 * h] = jnp.where(low, kg, lane_swap(vg)).astype(BF)
        out_ref[2 * h + 1] = jnp.where(low, lane_swap(kg), vg).astype(BF)


def sum_by_task(meta, ids, incoming, after):
    return pl.pallas_call(
        tasks_kernel,
        in_specs=[SMEM] * 5 + [VMEM] + [ANY] * 3,
        out_specs=VMEM,
        out_shape=jax.ShapeDtypeStruct((NZ, NTASK, ROWS, 2 * COLS), BF),
        scratch_shapes=[pltpu.VMEM((NTASK, NZ, ROWS, 2 * COLS), F32)],
        name="by_task",
        compiler_params=params(24),
    )(meta, *in_hbm(*ids), held(incoming), *in_hbm(*after))


def halves(a):
    high = a.astype(BF)
    return high, (a - high.astype(F32)).astype(BF)


def rows_kernel(in_ref, key_ref, value_ref, out_ref):
    grads = in_ref[0].astype(F32)
    for k in range(1, NZ):
        grads += in_ref[k].astype(F32)
    order = task_major()
    left = jnp.concatenate([dot(order, part, 0, 0).astype(BF) for part in halves(grads)], axis=1)
    for k in range(NXY):
        at = slice(k * SPAN, (k + 1) * SPAN)
        keys, values = key_ref[:, at], value_ref[:, at]
        weight = jnp.concatenate([keys, values, keys, values], axis=0)
        out_ref[k] = dot(left, weight, 1, 0).astype(BF)


def row_terms(parts, key_weight, value_weight):
    return pl.pallas_call(
        rows_kernel,
        in_specs=[VMEM] * 3,
        out_specs=VMEM,
        out_shape=jax.ShapeDtypeStruct((NXY, TROWS, SPAN), BF),
        name="row_terms",
        compiler_params=params(24),
    )(*held(parts, key_weight, value_weight))


WBLOCK = COLS + 4 * NTASK
PAIRS = 2 * NTASK


def partial_kernel(meta, in_ref, *refs):
    prompts, (out_ref, part_ref) = refs[:NZ], refs[NZ:]
    total = in_ref[0].astype(F32)
    for k in range(1, NXY):
        total += in_ref[k].astype(F32)
    out_ref[:, :COLS] = total.T.astype(BF).reshape(NZ, COLS, TROWS)
    low = iota((TROWS, 2 * COLS), 1) < COLS
    for k in range(NZ // 2):
        pair = total[:, 2 * COLS * k : 2 * COLS * (k + 1)]
        part_ref[2 * k] = jnp.where(low, pair, 0.0)
        part_ref[2 * k + 1] = jnp.where(low, lane_swap(pair), 0.0)
    shift = [0, NZ - 1, 1, NZ - 2, 2, NZ - 3, 3, NZ - 4]
    sums = jnp.zeros((2 * PAIRS, 2 * NSRC), F32)
    for first in range(0, NZ, 4):
        parts = [part_ref[lax.rem(meta[2] + shift[k], NZ)] for k in range(first, first + 4)]
        left = jnp.concatenate([parts[k] + lane_swap(parts[k + 1]) for k in (0, 2)], axis=1)
        high, rest = halves(left)
        for p in range(0, ROWS, 2):
            at = slice(p * NTASK, p * NTASK + PAIRS)
            rows = jnp.concatenate([high[at], rest[at]], axis=0)
            columns = [
                jnp.concatenate([prompts[k][p + i] for k in range(first, first + 4)], axis=0)
                for i in range(2)
            ]
            sums += dot(rows, jnp.concatenate(columns, axis=1), 1, 0)
    weight = sums[:NTASK, :NSRC] + sums[NTASK:PAIRS, NSRC:]
    weight += sums[PAIRS : PAIRS + NTASK, :NSRC] + sums[PAIRS + NTASK :, NSRC:]
    high = weight.astype(BF).astype(F32)
    middle = (weight - high).astype(BF).astype(F32)
    terms = [high, middle, weight - high - middle, jnp.zeros_like(weight)]
    terms = jnp.concatenate(terms, axis=0).astype(BF)
    for k in range(NZ):
        out_ref[k, COLS:] = terms


def partial_sums(meta, terms, prompts):
    return pl.pallas_call(
        partial_kernel,
        in_specs=[SMEM] + [VMEM] * (1 + NZ),
        out_specs=VMEM,
        out_shape=jax.ShapeDtypeStruct((NZ, WBLOCK, TROWS), BF),
        scratch_shapes=[pltpu.VMEM((NZ, TROWS, 2 * COLS), F32)],
        name="partial_sums",
        compiler_params=params(24),
    )(meta, *held(terms, *prompts))


def tile_kernel(in_ref, tile_ref, weight_ref):
    total = in_ref[0].astype(F32)
    for k in range(1, NZ):
        total += in_ref[k].astype(F32)
    tile_ref[...] = total[:COLS]
    high, middle, low = (total[COLS + k * NTASK : COLS + (k + 1) * NTASK] for k in range(3))
    weight = high + (middle + low)
    for k in range(GROUPS * NXY):
        weight_ref[k] = weight


def tile_sums(parts):
    return pl.pallas_call(
        tile_kernel,
        in_specs=[VMEM],
        out_specs=[VMEM, VMEM],
        out_shape=[
            pltpu.VMEM((COLS, TROWS), F32),
            jax.ShapeDtypeStruct((GROUPS * NXY, NTASK, NSRC), F32),
        ],
        name="tile_sums",
        compiler_params=params(24),
    )(held(parts))


def source_kernel(mix_ref, tile_ref, out_ref):
    spread = (iota((NTASK, TROWS), 0) == lane_task((NTASK, TROWS))).astype(BF)
    mix_high, mix_low = (dot(spread, m, 0, 0).astype(BF) for m in halves(mix_ref[...]))
    tile = tile_ref[...]
    row = iota((COLS, TROWS), 1) // NTASK
    for p in range(ROWS):
        high, low = halves(jnp.where(row == p, tile, 0.0))
        out_ref[p] = dot(high, mix_high, 1, 0) + dot(high, mix_low, 1, 0) + dot(low, mix_high, 1, 0)


def source_part(mix, tile):
    return pl.pallas_call(
        source_kernel,
        in_specs=[VMEM, VMEM],
        out_specs=VMEM,
        out_shape=jax.ShapeDtypeStruct((ROWS, COLS, NSRC), F32),
        name="source_part",
        compiler_params=params(24),
    )(*held(mix, tile))


def exchange(blocks, axes):
    return lax.all_to_all(blocks, axes, split_axis=0, concat_axis=0, tiled=True)


def from_peers(array, axes, members):
    got = [array]
    for k in range(1, members):
        got.append(lax.ppermute(array, axes, [(i, i ^ k) for i in range(members)]))
    return got


def ring_step(array, step):
    return lax.ppermute(array, "mp_2", [(i, (i + step) % NZ) for i in range(NZ)])


def on_device(
    source_prompts,
    task_logits,
    task_ids,
    key_weight,
    value_weight,
    queries,
    keys,
    values,
    cotangent,
):
    meta = jnp.stack([lax.axis_index(DP), lax.axis_index(XY), lax.axis_index("mp_2")])
    meta = meta.astype(jnp.int32)
    prompts_in = source_prompts.transpose(1, 2, 0)
    key_in, value_in = key_weight.T, value_weight.T
    mix, copies, rows = make_mixture(meta, task_logits, prompts_in)
    span = exchange(copies, "mp_2").reshape(SPAN, TROWS)

    def swap(array, k):
        return lax.ppermute(array, XY, [(i, i ^ k) for i in range(NXY)])

    blocks = {0: span}
    for k in (2, 4, 5, 7, 1, 3):
        blocks[k] = swap(span, k)
    blocks[6] = swap(blocks[2], 4)
    blocks = [blocks[k] for k in range(NXY)]
    around = [ring_step(rows, 1), ring_step(rows, -1)]
    copies = project(meta, blocks, key_in, value_in, around[:2])
    copies, task_ids = lax.optimization_barrier((copies, task_ids))
    ids = from_peers(task_ids, DP, GROUPS)
    gathered = exchange(copies, "mp_2").reshape(NZ, NTASK, ROWS, 2 * COLS)
    outgoing = select_prompts(meta, ids, gathered)
    stats = own_stats(outgoing, queries, keys, values, cotangent)
    around += [ring_step(around[0], 1), ring_step(around[1], -1)]
    prompts = exchange(outgoing, XYC).reshape(GROUPS, NXY, NZ, ROWS, DH)
    grads, norms = prompt_grads(around[2:4], prompts, stats, queries, cotangent)
    around += [ring_step(around[2], 1), ring_step(around[3], -1)]
    incoming = exchange(grads.reshape(GROUPS * NXY, NZ, ROWS, DH), XYC)
    attended = attention_output(prompts, norms, queries, keys, values)
    by_task = sum_by_task(meta, ids, incoming, [attended, *around[4:6]])
    around += [ring_step(around[4], 1)]
    parts = exchange(by_task.reshape(NZ, TROWS, 2 * COLS), "mp_2")
    terms = exchange(row_terms(parts, key_in, value_in), XY)
    terms = exchange(partial_sums(meta, terms, [rows, *around]), "mp_2")
    tile, spread = tile_sums(terms)
    weight_grad = exchange(spread, XYC).sum(axis=0)
    source_grad = source_part(mix, tile).transpose(2, 0, 1)
    logits_grad = mix * (weight_grad - jnp.sum(mix * weight_grad, axis=1, keepdims=True))
    return (attended, source_grad, logits_grad)


def solution(mesh):
    torus = Mesh(mesh.devices.reshape(2, 2, 2, 4, 8), DP_MP)
    return jax.shard_map(
        on_device,
        mesh=torus,
        in_specs=(
            P(None, None, MP),
            P(),
            P(DP),
            P(None, MP),
            P(None, MP),
            P(DP_MP, None, None),
            P(DP_MP, None, None),
            P(DP_MP, None, None),
            P(DP_MP, None, None),
        ),
        out_specs=(P(DP_MP, None, None), P(None, DP, MP), P()),
        check_vma=False,
    )
```

```python
import jax
import jax.numpy as jnp
from jax import lax
from jax.experimental import pallas as pl
from jax.experimental.pallas import tpu as pltpu
from jax.sharding import Mesh
from jax.sharding import PartitionSpec as P

D = 4096
HEADS = 32
DH = 128
NSRC = 128
NTASK = 8
PTOK = 64
SEQ = 128
DP = ("dp_0", "dp_1")
MP = ("mp_0", "mp_1", "mp_2")
DP_MP = ("dp_0", "dp_1", "mp_0", "mp_1", "mp_2")
XY = ("mp_0", "mp_1")
XYC = ("dp_0", "dp_1", "mp_0", "mp_1")
GROUPS = 4
ROWS = PTOK // GROUPS
NXY = 8
NZ = 8
COLS = D // (NXY * NZ)
TROWS = NTASK * ROWS
SPAN = NZ * COLS
BF = jnp.bfloat16
F32 = jnp.float32


SMEM = pl.BlockSpec(memory_space=pltpu.SMEM)
VMEM = pl.BlockSpec(memory_space=pltpu.VMEM)
ANY = pl.BlockSpec(memory_space=pl.ANY)


def dot(a, b, ca, cb):
    return lax.dot_general(a, b, (((ca,), (cb,)), ((), ())), preferred_element_type=F32)


def held(*arrays):
    kept = [pltpu.with_memory_space_constraint(a, pltpu.VMEM) for a in arrays]
    return kept if len(kept) > 1 else kept[0]


def in_hbm(*arrays):
    return [pltpu.with_memory_space_constraint(a, pltpu.HBM) for a in arrays]


def params(mib):
    return pltpu.CompilerParams(vmem_limit_bytes=mib * 2**20)


def iota(shape, axis):
    return lax.broadcasted_iota(jnp.int32, shape, axis)


def lane_swap(a):
    return pltpu.roll(a, COLS, a.ndim - 1)


def lane_task(shape):
    return iota(shape, 1) % NTASK


def mixture_kernel(meta, logits_ref, prompts_ref, mix_ref, out_ref, rows_ref):
    rows_ref[...] = prompts_ref[...]
    logits = logits_ref[...]
    exponent = jnp.exp(logits - jnp.max(logits, axis=1, keepdims=True))
    mix = exponent / jnp.sum(exponent, axis=1, keepdims=True)
    mix_ref[...] = mix
    spread = (iota((NTASK, TROWS), 0) == lane_task((NTASK, TROWS))).astype(BF)
    by_lane = dot(mix.astype(BF), spread, 0, 0).astype(BF)
    rows = prompts_ref[...].reshape(ROWS * COLS, NSRC)
    every = dot(rows, by_lane, 1, 0)
    row = iota((COLS, TROWS), 1) // NTASK
    mixture = every[:COLS]
    for p in range(1, ROWS):
        mixture = jnp.where(row == p, every[p * COLS : (p + 1) * COLS], mixture)
    mixture = mixture.astype(BF)
    for k in range(NZ):
        out_ref[k] = mixture


def make_mixture(meta, logits, prompts):
    return pl.pallas_call(
        mixture_kernel,
        grid_spec=pltpu.PrefetchScalarGridSpec(
            num_scalar_prefetch=1,
            grid=(1,),
            in_specs=[
                pl.BlockSpec((NTASK, NSRC), lambda i, m: (0, 0)),
                pl.BlockSpec((ROWS, COLS, NSRC), lambda i, m: (m[0], 0, 0)),
            ],
            out_specs=[
                pl.BlockSpec((NTASK, NSRC), lambda i, m: (0, 0)),
                pl.BlockSpec((NZ, COLS, TROWS), lambda i, m: (0, 0, 0)),
                pl.BlockSpec((ROWS, COLS, NSRC), lambda i, m: (0, 0, 0)),
            ],
        ),
        out_shape=[
            pltpu.VMEM((NTASK, NSRC), F32),
            jax.ShapeDtypeStruct((NZ, COLS, TROWS), BF),
            jax.ShapeDtypeStruct((ROWS, COLS, NSRC), BF),
        ],
        name="mixture",
        compiler_params=params(24),
    )(meta, *in_hbm(logits, prompts))


def task_major():
    r, c = iota((TROWS, TROWS), 0), iota((TROWS, TROWS), 1)
    return ((r % ROWS == c // NTASK) & (r // ROWS == c % NTASK)).astype(BF)


def project_kernel(meta, *refs):
    blocks, (key_ref, value_ref, out_ref) = refs[:NXY], refs[NXY + 2 :]
    total = jnp.zeros((2 * COLS, TROWS), F32)
    for k in range(NXY):
        start = pl.multiple_of((meta[1] ^ k) * SPAN, SPAN)
        weight = jnp.concatenate(
            [key_ref[:, pl.ds(start, SPAN)], value_ref[:, pl.ds(start, SPAN)]], axis=0
        )
        total += dot(weight, blocks[k][...], 1, 0)
    rows = dot(task_major(), total.astype(BF), 1, 1).astype(BF)
    for k in range(NZ):
        out_ref[k] = rows


def project(meta, blocks, key_weight, value_weight, after):
    return pl.pallas_call(
        project_kernel,
        in_specs=[SMEM] + [VMEM] * NXY + [ANY] * 2 + [VMEM] * 2,
        out_specs=VMEM,
        out_shape=jax.ShapeDtypeStruct((NZ, TROWS, 2 * COLS), BF),
        name="project",
        compiler_params=params(24),
    )(meta, *held(*blocks), *in_hbm(*after), *held(key_weight, value_weight))


def select_kernel(meta, i0, i1, i2, i3, in_ref, out_ref, table_ref):
    low = iota((NTASK, ROWS, 2 * COLS), 2) < COLS
    for h in range(NZ // 2):
        even = in_ref[2 * h].astype(F32)
        odd = in_ref[2 * h + 1].astype(F32)
        table_ref[:, h] = jnp.where(low, even, lane_swap(odd)).astype(BF)
        table_ref[:, NZ // 2 + h] = jnp.where(low, lane_swap(even), odd).astype(BF)
    group, z = meta[0], meta[2]
    for k, ids in enumerate((i0, i1, i2, i3)):
        for j in range(NXY):
            out_ref[(group ^ k) * NXY + j] = table_ref[ids[j * NZ + z]]


def select_prompts(meta, ids, gathered):
    return pl.pallas_call(
        select_kernel,
        in_specs=[SMEM] * 5 + [VMEM],
        out_specs=VMEM,
        out_shape=jax.ShapeDtypeStruct((GROUPS * NXY, NZ, ROWS, 2 * COLS), BF),
        scratch_shapes=[pltpu.VMEM((NTASK, NZ, ROWS, 2 * COLS), BF)],
        name="select",
        compiler_params=params(24),
    )(meta, *in_hbm(*ids), held(gathered))


HEADS_AT_ONCE = 16
XY_AT_ONCE = HEADS_AT_ONCE * NXY // HEADS
SCALE = DH ** (-0.5)


def own_scores(k_ref, q_ref, at):
    visible = iota((SEQ, SEQ), 0) <= iota((SEQ, SEQ), 1)
    return jnp.where(visible, dot(k_ref[:, at], q_ref[:, at], 1, 1) * SCALE, -1e30)


def head_lanes():
    return [slice(h * DH, (h + 1) * DH) for h in range(HEADS_AT_ONCE)]


def prompt_part(prompt_ref, h, value):
    per = NZ // 2
    at = pl.program_id(0) * XY_AT_ONCE + h // per
    return prompt_ref[:, at, value * per + h % per].reshape(PTOK, DH)


def own_kernel(after_ref, q_ref, k_ref, v_ref, c_ref, stat_ref, s_ref, g_ref):
    del after_ref
    for h, at in enumerate(head_lanes()):
        s_ref[h] = own_scores(k_ref, q_ref, at)
        g_ref[h] = dot(v_ref[:, at], c_ref[:, at], 1, 1)
    for h in range(HEADS_AT_ONCE):
        scores = s_ref[h]
        top = jnp.max(scores, axis=0, keepdims=True)
        exponent = jnp.exp(scores - top)
        total = jnp.sum(exponent, axis=0, keepdims=True)
        inner = jnp.sum(exponent * g_ref[h], axis=0, keepdims=True)
        stat_ref[h] = jnp.concatenate([top, total, inner, jnp.zeros((5, SEQ), F32)], axis=0)


def grads_kernel(
    after0, after1, prompt_ref, stat_ref, q_ref, c_ref, grad_ref, norm_ref, s_ref, g_ref, p_ref, d_ref
):
    del after0, after1
    for h, at in enumerate(head_lanes()):
        s_ref[h] = dot(prompt_part(prompt_ref, h, 0), q_ref[:, at], 1, 1) * SCALE
        g_ref[h] = dot(prompt_part(prompt_ref, h, 1), c_ref[:, at], 1, 1)
    for h in range(HEADS_AT_ONCE):
        own_top, own_total, own_inner = (stat_ref[h, i : i + 1] for i in range(3))
        scores, grads = s_ref[h], g_ref[h]
        top = jnp.maximum(jnp.max(scores, axis=0, keepdims=True), own_top)
        exponent = jnp.exp(scores - top)
        own = jnp.exp(own_top - top)
        share = 1.0 / (jnp.sum(exponent, axis=0, keepdims=True) + own * own_total)
        attn = exponent * share
        inner = jnp.sum(attn * grads, axis=0, keepdims=True) + own_inner * (own * share)
        p_ref[h] = attn.astype(BF)
        d_ref[h] = (attn * (grads - inner)).astype(BF)
        norm_ref[h] = jnp.concatenate([top, share, jnp.zeros((6, SEQ), F32)], axis=0)
    per = NZ // 2
    for h, at in enumerate(head_lanes()):
        kg = (dot(d_ref[h], q_ref[:, at], 1, 0) * SCALE).astype(BF)
        vg = dot(p_ref[h], c_ref[:, at], 1, 0).astype(BF)
        grad_ref[:, h // per, h % per] = kg.reshape(GROUPS, ROWS, DH)
        grad_ref[:, h // per, per + h % per] = vg.reshape(GROUPS, ROWS, DH)


def output_kernel(prompt_ref, norm_ref, q_ref, k_ref, v_ref, att_ref, s_ref, p_ref):
    for h, at in enumerate(head_lanes()):
        s_ref[h, :PTOK] = dot(prompt_part(prompt_ref, h, 0), q_ref[:, at], 1, 1) * SCALE
        s_ref[h, PTOK:] = own_scores(k_ref, q_ref, at)
    for h in range(HEADS_AT_ONCE):
        top, share = norm_ref[h, 0:1], norm_ref[h, 1:2]
        p_ref[h] = (jnp.exp(s_ref[h] - top) * share).astype(BF)
    for h, at in enumerate(head_lanes()):
        att = dot(p_ref[h, :PTOK], prompt_part(prompt_ref, h, 1), 0, 0)
        att += dot(p_ref[h, PTOK:], v_ref[:, at], 0, 0)
        att_ref[:, at] = att.astype(BF)


def attention_specs():
    seq = pl.BlockSpec((None, SEQ, DH * HEADS_AT_ONCE), lambda i: (0, 0, i))
    pair = pl.BlockSpec((GROUPS, XY_AT_ONCE, NZ, ROWS, DH), lambda i: (0, i, 0, 0, 0))
    stat = pl.BlockSpec((HEADS_AT_ONCE, 8, SEQ), lambda i: (i, 0, 0))
    return (HEADS // HEADS_AT_ONCE,), seq, pair, stat


def own_stats(after, queries, keys, values, cotangent):
    grid, seq, _, stat = attention_specs()
    square = pltpu.VMEM((HEADS_AT_ONCE, SEQ, SEQ), F32)
    return pl.pallas_call(
        own_kernel,
        grid=grid,
        in_specs=[ANY] + [seq] * 4,
        out_specs=stat,
        out_shape=jax.ShapeDtypeStruct((HEADS, 8, SEQ), F32),
        scratch_shapes=[square, square],
        name="own_stats",
        compiler_params=params(24),
    )(*in_hbm(after), queries, keys, values, cotangent)


def prompt_grads(after, prompts, stats, queries, cotangent):
    grid, seq, pair, stat = attention_specs()
    wide = (HEADS_AT_ONCE, PTOK, SEQ)
    return pl.pallas_call(
        grads_kernel,
        grid=grid,
        in_specs=[ANY, ANY, VMEM, stat, seq, seq],
        out_specs=[pair, stat],
        out_shape=[
            pltpu.HBM((GROUPS, NXY, NZ, ROWS, DH), BF),
            pltpu.HBM((HEADS, 8, SEQ), F32),
        ],
        scratch_shapes=[
            pltpu.VMEM(wide, F32),
            pltpu.VMEM(wide, F32),
            pltpu.VMEM(wide, BF),
            pltpu.VMEM(wide, BF),
        ],
        name="prompt_grads",
        compiler_params=params(24),
    )(*in_hbm(*after), held(prompts), stats, queries, cotangent)


def attention_output(prompts, norms, queries, keys, values):
    grid, seq, _, stat = attention_specs()
    wide = (HEADS_AT_ONCE, PTOK + SEQ, SEQ)
    return pl.pallas_call(
        output_kernel,
        grid=grid,
        in_specs=[VMEM, stat, seq, seq, seq],
        out_specs=seq,
        out_shape=jax.ShapeDtypeStruct((1, SEQ, D), BF),
        scratch_shapes=[pltpu.VMEM(wide, F32), pltpu.VMEM(wide, BF)],
        name="attention_output",
        compiler_params=params(24),
    )(held(prompts), norms, queries, keys, values)


def tasks_kernel(meta, i0, i1, i2, i3, in_ref, after0, after1, after2, out_ref, total_ref):
    del after0, after1, after2
    total_ref[...] = jnp.zeros_like(total_ref)
    group, z = meta[0], meta[2]
    for k, ids in enumerate((i0, i1, i2, i3)):
        for j in range(NXY):
            total_ref[ids[j * NZ + z]] += in_ref[(group ^ k) * NXY + j].astype(F32)
    low = iota((NTASK, ROWS, 2 * COLS), 2) < COLS
    for h in range(NZ // 2):
        kg, vg = total_ref[:, h], total_ref[:, NZ // 2 + h]
        out_ref[2 * h] = jnp.where(low, kg, lane_swap(vg)).astype(BF)
        out_ref[2 * h + 1] = jnp.where(low, lane_swap(kg), vg).astype(BF)


def sum_by_task(meta, ids, incoming, after):
    return pl.pallas_call(
        tasks_kernel,
        in_specs=[SMEM] * 5 + [VMEM] + [ANY] * 3,
        out_specs=VMEM,
        out_shape=jax.ShapeDtypeStruct((NZ, NTASK, ROWS, 2 * COLS), BF),
        scratch_shapes=[pltpu.VMEM((NTASK, NZ, ROWS, 2 * COLS), F32)],
        name="by_task",
        compiler_params=params(24),
    )(meta, *in_hbm(*ids), held(incoming), *in_hbm(*after))


def halves(a):
    high = a.astype(BF)
    return high, (a - high.astype(F32)).astype(BF)


def rows_kernel(meta, in_ref, key_ref, value_ref, *out_refs):
    grads = in_ref[0].astype(F32)
    for k in range(1, NZ):
        grads += in_ref[k].astype(F32)
    order = task_major()
    left = jnp.concatenate([dot(order, part, 0, 0).astype(BF) for part in halves(grads)], axis=1)
    for k in range(NXY):
        at = pl.ds(pl.multiple_of((meta[1] ^ k) * SPAN, SPAN), SPAN)
        keys, values = key_ref[:, at], value_ref[:, at]
        weight = jnp.concatenate([keys, values, keys, values], axis=0)
        out_refs[k][...] = dot(left, weight, 1, 0).astype(BF)


def row_terms(meta, parts, key_weight, value_weight):
    return pl.pallas_call(
        rows_kernel,
        in_specs=[SMEM] + [VMEM] * 3,
        out_specs=[VMEM] * NXY,
        out_shape=[pltpu.VMEM((TROWS, SPAN), BF)] * NXY,
        name="row_terms",
        compiler_params=params(24),
    )(meta, *held(parts, key_weight, value_weight))


WBLOCK = COLS + 4 * NTASK
PAIRS = 2 * NTASK


def partial_kernel(meta, *refs):
    terms, prompts, (out_ref, part_ref) = refs[: NXY - 1], refs[NXY - 1 : -2], refs[-2:]
    total = terms[0][...].astype(F32)
    for term in terms[1:]:
        total += term[...].astype(F32)
    out_ref[:, :COLS] = total.T.astype(BF).reshape(NZ, COLS, TROWS)
    low = iota((TROWS, 2 * COLS), 1) < COLS
    for k in range(NZ // 2):
        pair = total[:, 2 * COLS * k : 2 * COLS * (k + 1)]
        part_ref[2 * k] = jnp.where(low, pair, 0.0)
        part_ref[2 * k + 1] = jnp.where(low, lane_swap(pair), 0.0)
    shift = [0, NZ - 1, 1, NZ - 2, 2, NZ - 3, 3, NZ - 4]
    sums = jnp.zeros((2 * PAIRS, 2 * NSRC), F32)
    for first in range(0, NZ, 4):
        parts = [part_ref[lax.rem(meta[2] + shift[k], NZ)] for k in range(first, first + 4)]
        left = jnp.concatenate([parts[k] + lane_swap(parts[k + 1]) for k in (0, 2)], axis=1)
        high, rest = halves(left)
        for p in range(0, ROWS, 2):
            at = slice(p * NTASK, p * NTASK + PAIRS)
            rows = jnp.concatenate([high[at], rest[at]], axis=0)
            columns = [
                jnp.concatenate([prompts[k][p + i] for k in range(first, first + 4)], axis=0)
                for i in range(2)
            ]
            sums += dot(rows, jnp.concatenate(columns, axis=1), 1, 0)
    weight = sums[:NTASK, :NSRC] + sums[NTASK:PAIRS, NSRC:]
    weight += sums[PAIRS : PAIRS + NTASK, :NSRC] + sums[PAIRS + NTASK :, NSRC:]
    high = weight.astype(BF).astype(F32)
    middle = (weight - high).astype(BF).astype(F32)
    terms = [high, middle, weight - high - middle, jnp.zeros_like(weight)]
    terms = jnp.concatenate(terms, axis=0).astype(BF)
    for k in range(NZ):
        out_ref[k, COLS:] = terms


def partial_sums(meta, terms, prompts):
    return pl.pallas_call(
        partial_kernel,
        in_specs=[SMEM] + [VMEM] * (NXY - 1 + NZ),
        out_specs=VMEM,
        out_shape=jax.ShapeDtypeStruct((NZ, WBLOCK, TROWS), BF),
        scratch_shapes=[pltpu.VMEM((NZ, TROWS, 2 * COLS), F32)],
        name="partial_sums",
        compiler_params=params(24),
    )(meta, *held(*terms, *prompts))


def tile_kernel(in_ref, tile_ref, weight_ref):
    total = in_ref[0].astype(F32)
    for k in range(1, NZ):
        total += in_ref[k].astype(F32)
    tile_ref[...] = total[:COLS]
    high, middle, low = (total[COLS + k * NTASK : COLS + (k + 1) * NTASK] for k in range(3))
    weight = high + (middle + low)
    for k in range(GROUPS * NXY):
        weight_ref[k] = weight


def tile_sums(parts):
    return pl.pallas_call(
        tile_kernel,
        in_specs=[VMEM],
        out_specs=[VMEM, VMEM],
        out_shape=[
            pltpu.VMEM((COLS, TROWS), F32),
            jax.ShapeDtypeStruct((GROUPS * NXY, NTASK, NSRC), F32),
        ],
        name="tile_sums",
        compiler_params=params(24),
    )(held(parts))


def source_kernel(mix_ref, tile_ref, out_ref):
    spread = (iota((NTASK, TROWS), 0) == lane_task((NTASK, TROWS))).astype(BF)
    mix_high, mix_low = (dot(spread, m, 0, 0).astype(BF) for m in halves(mix_ref[...]))
    tile = tile_ref[...]
    row = iota((COLS, TROWS), 1) // NTASK
    for p in range(ROWS):
        high, low = halves(jnp.where(row == p, tile, 0.0))
        out_ref[p] = dot(high, mix_high, 1, 0) + dot(high, mix_low, 1, 0) + dot(low, mix_high, 1, 0)


def source_part(mix, tile):
    return pl.pallas_call(
        source_kernel,
        in_specs=[VMEM, VMEM],
        out_specs=VMEM,
        out_shape=jax.ShapeDtypeStruct((ROWS, COLS, NSRC), F32),
        name="source_part",
        compiler_params=params(24),
    )(*held(mix, tile))


def exchange(blocks, axes):
    return lax.all_to_all(blocks, axes, split_axis=0, concat_axis=0, tiled=True)


def from_peers(array, axes, members):
    got = [array]
    for k in range(1, members):
        got.append(lax.ppermute(array, axes, [(i, i ^ k) for i in range(members)]))
    return got


def ring_step(array, step):
    return lax.ppermute(array, "mp_2", [(i, (i + step) % NZ) for i in range(NZ)])


def on_device(
    source_prompts,
    task_logits,
    task_ids,
    key_weight,
    value_weight,
    queries,
    keys,
    values,
    cotangent,
):
    meta = jnp.stack([lax.axis_index(DP), lax.axis_index(XY), lax.axis_index("mp_2")])
    meta = meta.astype(jnp.int32)
    prompts_in = source_prompts.transpose(1, 2, 0)
    key_in, value_in = key_weight.T, value_weight.T
    mix, copies, rows = make_mixture(meta, task_logits, prompts_in)
    span = exchange(copies, "mp_2").reshape(SPAN, TROWS)

    def swap(array, k):
        return lax.ppermute(array, XY, [(i, i ^ k) for i in range(NXY)])

    blocks = {0: span}
    for k in (2, 4, 5, 7, 1, 3):
        blocks[k] = swap(span, k)
    blocks[6] = swap(blocks[2], 4)
    blocks = [blocks[k] for k in range(NXY)]
    around = [ring_step(rows, 1), ring_step(rows, -1)]
    copies = project(meta, blocks, key_in, value_in, around[:2])
    copies, task_ids = lax.optimization_barrier((copies, task_ids))
    ids = from_peers(task_ids, DP, GROUPS)
    gathered = exchange(copies, "mp_2").reshape(NZ, NTASK, ROWS, 2 * COLS)
    outgoing = select_prompts(meta, ids, gathered)
    stats = own_stats(outgoing, queries, keys, values, cotangent)
    around += [ring_step(around[0], 1), ring_step(around[1], -1)]
    prompts = exchange(outgoing, XYC).reshape(GROUPS, NXY, NZ, ROWS, DH)
    grads, norms = prompt_grads(around[2:4], prompts, stats, queries, cotangent)
    around += [ring_step(around[2], 1), ring_step(around[3], -1)]
    incoming = exchange(grads.reshape(GROUPS * NXY, NZ, ROWS, DH), XYC)
    attended = attention_output(prompts, norms, queries, keys, values)
    by_task = sum_by_task(meta, ids, incoming, [attended, *around[4:6]])
    around += [ring_step(around[4], 1)]
    parts = exchange(by_task.reshape(NZ, TROWS, 2 * COLS), "mp_2")
    terms = row_terms(meta, parts, key_in, value_in)
    joined = swap(terms[6], 4)
    arrived = [swap(terms[k], k) for k in (4, 5, 7, 1, 3)]
    joined = (terms[2].astype(F32) + joined.astype(F32)).astype(BF)
    terms = [terms[0], *arrived, swap(joined, 2)]
    terms = exchange(partial_sums(meta, terms, [rows, *around]), "mp_2")
    tile, spread = tile_sums(terms)
    weight_grad = exchange(spread, XYC).sum(axis=0)
    source_grad = source_part(mix, tile).transpose(2, 0, 1)
    logits_grad = mix * (weight_grad - jnp.sum(mix * weight_grad, axis=1, keepdims=True))
    return (attended, source_grad, logits_grad)


def solution(mesh):
    torus = Mesh(mesh.devices.reshape(2, 2, 2, 4, 8), DP_MP)
    return jax.shard_map(
        on_device,
        mesh=torus,
        in_specs=(
            P(None, None, MP),
            P(),
            P(DP),
            P(None, MP),
            P(None, MP),
            P(DP_MP, None, None),
            P(DP_MP, None, None),
            P(DP_MP, None, None),
            P(DP_MP, None, None),
        ),
        out_specs=(P(DP_MP, None, None), P(None, DP, MP), P()),
        check_vma=False,
    )
```
